32 devices in a mesh: dz: 4 (over z), dy: 2 (over y), dx: 4 (over x, core).
Axes of the slice: x: 2, y: 2, z: 4, core: 2. Of those that a mesh axis runs over, the one named last changes fastest.
Arguments:
- act_one: bfloat16 [65536, 1024], P(('dz', 'dy', 'dx'))
- pre_one: bfloat16 [65536, 4096], P(('dz', 'dy', 'dx'))
- act_two: bfloat16 [65536, 1024], P(('dz', 'dy', 'dx'))
- pre_two: bfloat16 [65536, 4096], P(('dz', 'dy', 'dx'))
- grad_out: bfloat16 [65536, 1024], P(('dz', 'dy', 'dx'))
- w_in_two: bfloat16 [1024, 4096], replicated
- w_out_one: bfloat16 [4096, 1024], replicated
- w_out_two: bfloat16 [4096, 1024], replicated
Outputs:
- output: float32 [16777216], P(('dx', 'dy', 'dz'))
All inputs are finite; a program needn't handle non-finite values.
Results may differ from the reference program's by a relative error of at most 0.00156588.
Values are sent between devices in bfloat16 or wider.
A program may use at most 1 GiB of HBM per device.

```python
import jax
import jax.numpy as jnp
from jax import lax

D = 1024
FF = 4096
TOKENS_DEV = 2048
N_DEVICES = 32
N_MICRO = 2


def setup_inputs(seed: int = 0) -> dict:
    key_list = jax.random.split(jax.random.key(seed), 8)
    row_count = N_DEVICES * TOKENS_DEV
    grad_scale = (N_DEVICES * TOKENS_DEV) ** -0.5
    drawn = {
        'act_one': jax.random.normal(key_list[0], (row_count, D), jnp.float32),
        'pre_one': jax.random.normal(key_list[1], (row_count, FF), jnp.float32),
        'act_two': jax.random.normal(key_list[2], (row_count, D), jnp.float32),
        'pre_two': jax.random.normal(key_list[3], (row_count, FF), jnp.float32),
        'grad_out': jax.random.normal(key_list[4], (row_count, D), jnp.float32) * grad_scale,
        'w_in_two': jax.random.normal(key_list[5], (D, FF), jnp.float32) * D ** -0.5,
        'w_out_one': jax.random.normal(key_list[6], (FF, D), jnp.float32) * FF ** -0.5,
        'w_out_two': jax.random.normal(key_list[7], (FF, D), jnp.float32) * FF ** -0.5,
    }
    return {key_name: drawn_val.astype(jnp.bfloat16) for key_name, drawn_val in drawn.items()}


def gelu_pair(pre):
    pre_wide = pre.astype(jnp.float32)
    hidden, pull_back = jax.vjp(jax.nn.gelu, pre_wide)
    return hidden, pull_back(jnp.ones_like(pre_wide))[0]


def micro_grads(act_one, pre_one, act_two, pre_two, grad_out, w_in_two, w_out_one, w_out_two):
    hid_two, slope_two = gelu_pair(pre_two)
    hid_two = hid_two.astype(jnp.bfloat16)
    g_out_two = jnp.dot(hid_two.T, grad_out, preferred_element_type=jnp.float32).astype(jnp.bfloat16)
    d_hid_two = jnp.dot(grad_out, w_out_two.T, preferred_element_type=jnp.float32)
    d_pre_two = (d_hid_two * slope_two).astype(jnp.bfloat16)
    g_in_two = jnp.dot(act_two.T, d_pre_two, preferred_element_type=jnp.float32).astype(jnp.bfloat16)
    d_back_two = jnp.dot(d_pre_two, w_in_two.T, preferred_element_type=jnp.float32)
    d_act_two = (grad_out.astype(jnp.float32) + d_back_two).astype(jnp.bfloat16)
    hid_one, slope_one = gelu_pair(pre_one)
    hid_one = hid_one.astype(jnp.bfloat16)
    g_out_one = jnp.dot(hid_one.T, d_act_two, preferred_element_type=jnp.float32).astype(jnp.bfloat16)
    d_hid_one = jnp.dot(d_act_two, w_out_one.T, preferred_element_type=jnp.float32)
    d_pre_one = (d_hid_one * slope_one).astype(jnp.bfloat16)
    g_in_one = jnp.dot(act_one.T, d_pre_one, preferred_element_type=jnp.float32).astype(jnp.bfloat16)
    return (g_out_two, g_in_two, g_out_one, g_in_one)


def reference(act_one, pre_one, act_two, pre_two, grad_out, w_in_two, w_out_one, w_out_two):
    micro_rows = TOKENS_DEV // N_MICRO
    batch_count = N_DEVICES * N_MICRO
    stacked = tuple(array_in.reshape(batch_count, micro_rows, array_in.shape[1]) for array_in in (act_one, pre_one, act_two, pre_two, grad_out))

    def scan_step(running, micro_slab):
        micro_out = micro_grads(*micro_slab, w_in_two, w_out_one, w_out_two)
        return tuple(run_sum + grad_piece.astype(jnp.float32) for run_sum, grad_piece in zip(running, micro_out)), None

    zero_sums = (jnp.zeros((FF, D), jnp.float32), jnp.zeros((D, FF), jnp.float32), jnp.zeros((FF, D), jnp.float32), jnp.zeros((D, FF), jnp.float32))
    grad_sums, _ = lax.scan(scan_step, zero_sums, stacked)
    return jnp.concatenate([grad_piece.reshape(-1) for grad_piece in grad_sums])
```

```python
import functools

import jax
import jax.numpy as jnp
from jax import lax
from jax.experimental import pallas as pl
from jax.experimental.pallas import tpu as pltpu
from jax.sharding import PartitionSpec as P

MESH = pl.DeviceIdType.MESH
F32 = jnp.float32
BF16 = jnp.bfloat16
N_CHUNK = 8
ROOT = 0.7978845608028654
CUBE = 0.044715


def gelu_hidden(pre):
    square = pre * pre
    bend = jnp.tanh(pre * (ROOT + (ROOT * CUBE) * square))
    half = 0.5 * pre
    return half + half * bend


def gelu_slope(pre):
    square = pre * pre
    bend = jnp.tanh(pre * (ROOT + (ROOT * CUBE) * square))
    tail = ((1.0 - bend * bend) * pre) * ((1.5 * ROOT * CUBE) * square + 0.5 * ROOT)
    return (0.5 + 0.5 * bend) + tail


def dot_nn(left, right):
    return lax.dot_general(left, right, (((1,), (0,)), ((), ())), preferred_element_type=F32)


def dot_nt(left, right):
    return lax.dot_general(left, right, (((1,), (1,)), ((), ())), preferred_element_type=F32)


class Dims:
    def __init__(self, tokens, width):
        self.tokens = tokens
        self.micro = tokens // 2
        self.width = width
        self.hidden = 4 * width
        self.rows = width // 8
        self.tile = 2 * self.rows
        self.half = width // 2
        unit = self.rows // 16
        self.row_a = max(8, (unit * 5) // 8 * 8)
        self.row_c = 4 * unit
        self.row_b = self.rows - self.row_a - self.row_c
        self.block = min(256, self.micro)
        self.span = min(512, width)


def kernel(dims, z2, z1, x2, x1, dy, win2, wo1, wo2, out,
           gin, xt, acc, dz, zbuf, wbuf, winbuf, ht, stage, rcore,
           s1, r1a, r1b, r1c, s2a, s2b, s2c, r2a, r2b, r2c, s3ab, s3c, r3ab, r3c, s4ab, s4c, r4ab, r4c, fin,
           zsem, wsem, winsem, xsem, gsem,
           core_send, core_recv, send1, recv1, send2, recv2, send3, recv3, send4, recv4,
           fin_send, fin_recv, fin_local, credit):
    rows, tile, width, half = dims.rows, dims.tile, dims.width, dims.half
    micro, tokens, block, span = dims.micro, dims.tokens, dims.block, dims.span
    row_a, row_b, row_c = dims.row_a, dims.row_b, dims.row_c
    row_ab = row_a + row_b
    iz, iy, ix = lax.axis_index('dz'), lax.axis_index('dy'), lax.axis_index('dx')
    px, core = ix // 2, ix % 2
    zhi, zlo = iz // 2, iz % 2
    to_core = (iz, iy, px * 2 + (1 - core))
    to_x = (iz, iy, (1 - px) * 2 + core)
    to_xc = (iz, iy, (1 - px) * 2 + (1 - core))
    to_y = (iz, 1 - iy, ix)
    to_za = (zhi * 2 + (1 - zlo), iy, ix)
    to_zb = ((1 - zhi) * 2 + zlo, iy, ix)
    keep_x = pl.ds(pl.multiple_of(px * half, 128), half)
    send_x = pl.ds(pl.multiple_of((1 - px) * half, 128), half)
    CORE, A1, B1, C1, A2, B2, C2, AB3, C3, AB4, C4 = range(11)

    barrier = pltpu.get_barrier_semaphore()
    for peer in (to_core, to_x, to_xc, to_y, to_za, to_zb):
        pl.semaphore_signal(barrier, inc=1, device_id=peer, device_id_type=MESH)

    def piece_start(num):
        k, s, p = num // 8, (num // 4) % 2, num % 4
        b, i, g = k // 4, (k // 2) % 2, k % 2
        j = 2 * i + jnp.where(s == 0, 1 - core, core)
        slot = num % 3

        def from_block(zref, wref):
            @pl.when(g == 0)
            def _():
                for h in range(2):
                    col = pl.multiple_of((dims.hidden // 8) * (2 * p + h) + rows * j, rows)
                    pltpu.make_async_copy(zref.at[:, pl.ds(col, rows)], zbuf.at[slot, :, pl.ds(h * rows, rows)], zsem.at[slot]).start()

            @pl.when(g == 1)
            def _():
                col = pl.multiple_of(width * j + tile * p, tile)
                pltpu.make_async_copy(zref.at[:, pl.ds(col, tile)], zbuf.at[slot], zsem.at[slot]).start()
                pltpu.make_async_copy(wref.at[pl.ds(col, tile), :], wbuf.at[slot], wsem.at[slot]).start()

        @pl.when(b == 0)
        def _():
            from_block(z2, wo2)

        @pl.when(b == 1)
        def _():
            from_block(z1, wo1)

    def piece_wait(num, with_w):
        slot = num % 3
        pltpu.make_async_copy(z2.at[:, pl.ds(0, tile)], zbuf.at[slot], zsem.at[slot]).wait()
        if with_w:
            pltpu.make_async_copy(wo2.at[pl.ds(0, tile), :], wbuf.at[slot], wsem.at[slot]).wait()

    def x_copy(xref):
        return pltpu.make_async_copy(xref, dz, xsem)

    def core_copy(p):
        return pltpu.make_async_remote_copy(stage.at[p % 2], rcore.at[p], core_send.at[p % 2], core_recv.at[p], device_id=to_core, device_id_type=MESH)

    def phase1(slot):
        return (
            pltpu.make_async_remote_copy(s1.at[slot, :, :, :, pl.ds(0, row_a), send_x], r1a.at[slot], send1.at[slot, 0], recv1.at[slot, 0], device_id=to_x, device_id_type=MESH),
            pltpu.make_async_remote_copy(s1.at[slot, 1 - iy, :, :, pl.ds(row_a, row_b), :], r1b.at[slot], send1.at[slot, 1], recv1.at[slot, 1], device_id=to_y, device_id_type=MESH),
            pltpu.make_async_remote_copy(s1.at[slot, :, :, 1 - zlo, pl.ds(row_ab, row_c), :], r1c.at[slot], send1.at[slot, 2], recv1.at[slot, 2], device_id=to_za, device_id_type=MESH),
        )

    def phase2():
        return (
            pltpu.make_async_remote_copy(s2a.at[1 - iy], r2a, send2.at[0], recv2.at[0], device_id=to_y, device_id_type=MESH),
            pltpu.make_async_remote_copy(s2b.at[:, :, :, send_x], r2b, send2.at[1], recv2.at[1], device_id=to_x, device_id_type=MESH),
            pltpu.make_async_remote_copy(s2c.at[:, 1 - zhi], r2c, send2.at[2], recv2.at[2], device_id=to_zb, device_id_type=MESH),
        )

    def phase3():
        return (
            pltpu.make_async_remote_copy(s3ab.at[:, 1 - zlo], r3ab, send3.at[0], recv3.at[0], device_id=to_za, device_id_type=MESH),
            pltpu.make_async_remote_copy(s3c.at[:, :, send_x], r3c, send3.at[1], recv3.at[1], device_id=to_x, device_id_type=MESH),
        )

    def phase4():
        return (
            pltpu.make_async_remote_copy(s4ab.at[1 - zhi], r4ab, send4.at[0], recv4.at[0], device_id=to_zb, device_id_type=MESH),
            pltpu.make_async_remote_copy(s4c.at[1 - iy], r4c, send4.at[1], recv4.at[1], device_id=to_y, device_id_type=MESH),
        )

    def grant(kind, peer, ok):
        @pl.when(ok)
        def _():
            pl.semaphore_signal(credit.at[kind], inc=1, device_id=peer, device_id_type=MESH)

    def claim(kind, ok):
        @pl.when(ok)
        def _():
            pl.semaphore_wait(credit.at[kind], 1)

    def out_place(i, c, x):
        return out.at[2 * i + c, :, pl.ds(pl.multiple_of(x * half, 128), half)]

    def fin_remote(chunk):
        b, i, g = chunk // 4, (chunk // 2) % 2, chunk % 2
        return pltpu.make_async_remote_copy(fin, out_place(i, core, px), fin_send, fin_recv.at[i, ix], device_id=(iz, iy, 2 * b + g), device_id_type=MESH)

    def fin_here(chunk):
        i = (chunk // 2) % 2
        return pltpu.make_async_copy(fin, out_place(i, core, px), fin_local)

    def owner_of(chunk):
        return 2 * (chunk // 4) + chunk % 2

    def fin_wait(chunk):
        @pl.when(owner_of(chunk) == ix)
        def _():
            fin_here(chunk).wait()

        @pl.when(owner_of(chunk) != ix)
        def _():
            fin_remote(chunk).wait_send()

    def service(k):
        @pl.when(jnp.logical_and(k >= 4, k < N_CHUNK + 4))
        def _():
            chunk = k - 4
            more = chunk < N_CHUNK - 1
            ab, c = phase4()

            @pl.when(chunk >= 1)
            def _():
                fin_wait(chunk - 1)
            ab.wait()
            fin[0:row_ab, :] = s4ab[zhi] + r4ab[...]
            grant(AB4, to_zb, more)
            c.wait()
            fin[row_ab:rows, :] = s4c[iy] + r4c[...]
            grant(C4, to_y, more)

            @pl.when(owner_of(chunk) == ix)
            def _():
                fin_here(chunk).start()

            @pl.when(owner_of(chunk) != ix)
            def _():
                fin_remote(chunk).start()

        @pl.when(jnp.logical_and(k >= 3, k < N_CHUNK + 3))
        def _():
            chunk = k - 3
            more, later = chunk < N_CHUNK - 1, chunk >= 1
            ab, c = phase3()
            ab4, c4 = phase4()
            ab.wait()
            s4ab[...] = s3ab[:, zlo] + r3ab[...]
            grant(AB3, to_za, more)
            claim(AB4, later)
            ab4.start()
            c.wait()
            s4c[...] = s3c[:, :, keep_x] + r3c[...]
            grant(C3, to_x, more)
            claim(C4, later)
            c4.start()

        @pl.when(jnp.logical_and(k >= 2, k < N_CHUNK + 2))
        def _():
            chunk = k - 2
            more, later = chunk < N_CHUNK - 1, chunk >= 1
            a, b, c = phase2()
            ab3, c3 = phase3()
            a.wait()
            s3ab[:, :, 0:row_a, :] = s2a[iy] + r2a[...]
            grant(A2, to_y, more)
            b.wait()
            s3ab[:, :, row_a:row_ab, :] = s2b[:, :, :, keep_x] + r2b[...]
            grant(B2, to_x, more)
            claim(AB3, later)
            ab3.start()
            c.wait()
            s3c[...] = s2c[:, zhi] + r2c[...]
            grant(C2, to_zb, more)
            claim(C3, later)
            c3.start()

        @pl.when(jnp.logical_and(k >= 1, k < N_CHUNK + 1))
        def _():
            chunk = k - 1
            slot = chunk % 2
            more, later = chunk < N_CHUNK - 2, chunk >= 1
            a, b, c = phase1(slot)
            a2, b2, c2 = phase2()
            a.wait()
            s2a[...] = s1[slot, :, :, :, 0:row_a, keep_x] + r1a[slot]
            grant(A1, to_x, more)
            claim(A2, later)
            a2.start()
            b.wait()
            s2b[...] = s1[slot, iy, :, :, row_a:row_ab, :] + r1b[slot]
            grant(B1, to_y, more)
            claim(B2, later)
            b2.start()
            c.wait()
            s2c[...] = s1[slot, :, :, zlo, row_ab:rows, :] + r1c[slot]
            grant(C1, to_za, more)
            claim(C2, later)
            c2.start()

    def emit_tile(k, s, p, cols, value):
        @pl.when(s == 0)
        def _():
            stage[p % 2, :, cols] = value

        @pl.when(s == 1)
        def _():
            total = value + rcore[p, :, cols]
            s1[k % 2, p // 2, p % 2, 0, :, cols] = total[0:rows]
            s1[k % 2, p // 2, p % 2, 1, :, cols] = total[rows:tile]

    def tile_open(k, s, p):
        @pl.when(s == 0)
        def _():
            @pl.when(p >= 2)
            def _():
                core_copy(p - 2).wait_send()

        @pl.when(s == 1)
        def _():
            core_copy(p).wait_recv()

    def tile_close(k, s, p):
        @pl.when(s == 0)
        def _():
            claim(CORE, k >= 1)
            core_copy(p).start()

        @pl.when(s == 1)
        def _():
            grant(CORE, to_core, k < N_CHUNK - 1)

    def drain_stage(s):
        @pl.when(s == 0)
        def _():
            core_copy(2).wait_send()
            core_copy(3).wait_send()

    def half_out(k, s):
        @pl.loop(0, 4)
        def _(p):
            num = k * 8 + s * 4 + p

            @pl.when(num + 2 < 64)
            def _():
                piece_start(num + 2)
            piece_wait(num, False)
            slot = num % 3
            for r in range(tokens // block):
                pre = zbuf[slot, r * block:(r + 1) * block, :].astype(F32)
                ht[:, r * block:(r + 1) * block] = gelu_hidden(pre).astype(BF16).T
            tile_open(k, s, p)
            for n in range(width // span):
                cols = slice(n * span, (n + 1) * span)
                value = None
                for m in range(2):
                    part = dot_nn(ht[:, m * micro:(m + 1) * micro], gin[m * micro:(m + 1) * micro, cols]).astype(BF16).astype(F32)
                    value = part if value is None else value + part
                emit_tile(k, s, p, cols, value)
            tile_close(k, s, p)
        drain_stage(s)

    def half_in(k, s):
        b, i = k // 4, (k // 2) % 2
        j = 2 * i + jnp.where(s == 0, 1 - core, core)

        @pl.when(b == 0)
        def _():
            pltpu.make_async_copy(win2.at[:, pl.ds(pl.multiple_of(width * j, width), width)], winbuf, winsem).start()

        @pl.loop(0, 4)
        def _(p):
            num = k * 8 + s * 4 + p

            @pl.when(num + 2 < 64)
            def _():
                piece_start(num + 2)
            piece_wait(num, True)
            slot = num % 3
            where = pl.ds(pl.multiple_of(p * tile, tile), tile)
            for r in range(tokens // block):
                part = slice(r * block, (r + 1) * block)
                back = dot_nt(gin[part, :], wbuf[slot])
                dz[part, where] = (back * gelu_slope(zbuf[slot, part, :].astype(F32))).astype(BF16)

        @pl.loop(0, 4)
        def _(p):
            lines = pl.ds(pl.multiple_of(p * tile, tile), tile)
            tile_open(k, s, p)
            for n in range(width // span):
                cols = slice(n * span, (n + 1) * span)
                value = None
                for m in range(2):
                    part = dot_nn(xt[lines, m * micro:(m + 1) * micro], dz[m * micro:(m + 1) * micro, cols]).astype(BF16).astype(F32)
                    value = part if value is None else value + part
                emit_tile(k, s, p, cols, value)
            tile_close(k, s, p)
        drain_stage(s)

    def pass_back(k):
        @pl.when(k // 4 == 0)
        def _():
            pltpu.make_async_copy(win2.at[:, pl.ds(0, width)], winbuf, winsem).wait()

            @pl.loop(0, width // tile)
            def _(n):
                lines = pl.ds(pl.multiple_of(n * tile, tile), tile)
                for m in range(2):
                    part = slice(m * micro, (m + 1) * micro)
                    acc[part, lines] += dot_nt(dz[part, :], winbuf[lines, :])

    piece_start(0)
    first = pltpu.make_async_copy(dy, gin, gsem)
    first.start()
    piece_start(1)
    x_copy(x2).start()
    first.wait()

    @pl.loop(0, tokens // block)
    def _(r):
        part = pl.ds(pl.multiple_of(r * block, block), block)
        acc[part, :] = gin[part, :].astype(F32)
    pl.semaphore_wait(barrier, 6)

    @pl.loop(0, N_CHUNK + 4)
    def _(k):
        @pl.when(k < N_CHUNK)
        def _():
            @pl.when(k == 4)
            def _():
                x_copy(x1).start()

                @pl.loop(0, tokens // block)
                def _(r):
                    part = pl.ds(pl.multiple_of(r * block, block), block)
                    gin[part, :] = acc[part, :].astype(BF16)

            @pl.when(k % 2 == 0)
            def _():
                @pl.loop(0, 2)
                def _(s):
                    half_out(k, s)

            @pl.when(k % 4 == 1)
            def _():
                x_copy(x2).wait()

                @pl.loop(0, tokens // block)
                def _(r):
                    part = pl.ds(pl.multiple_of(r * block, block), block)
                    for q in range(width // tile):
                        xt[q * tile:(q + 1) * tile, part] = dz[part, q * tile:(q + 1) * tile].T

            @pl.when(k % 2 == 1)
            def _():
                half_in(k, 0)
                pass_back(k)
                half_in(k, 1)

            claim(A1, k >= 2)
            claim(B1, k >= 2)
            claim(C1, k >= 2)
            for copy in phase1(k % 2):
                copy.start()

            @pl.when(k % 2 == 1)
            def _():
                pass_back(k)
        service(k)

    fin_wait(N_CHUNK - 1)
    for i in range(2):
        for d in range(4):
            @pl.when(ix != d)
            def _():
                place = out_place(i, d % 2, d // 2)
                pltpu.make_async_remote_copy(fin, place, fin_send, fin_recv.at[i, d], device_id=to_core, device_id_type=MESH).wait_recv()


def scratch(dims):
    t, w, r, h = dims.tokens, dims.width, dims.rows, dims.half
    a, b, c = dims.row_a, dims.row_b, dims.row_c
    tile = dims.tile
    V, DMA = pltpu.VMEM, pltpu.SemaphoreType.DMA
    return [
        V((t, w), BF16), V((w, t), BF16), V((t, w), F32), V((t, w), BF16), V((3, t, tile), BF16), V((3, tile, w), BF16), V((w, w), BF16),
        V((tile, t), BF16), V((2, tile, w), F32), V((4, tile, w), F32),
        V((2, 2, 2, 2, r, w), F32), V((2, 2, 2, 2, a, h), F32), V((2, 2, 2, b, w), F32), V((2, 2, 2, c, w), F32),
        V((2, 2, 2, a, h), F32), V((2, 2, b, w), F32), V((2, 2, c, w), F32),
        V((2, 2, a, h), F32), V((2, 2, b, h), F32), V((2, c, w), F32),
        V((2, 2, a + b, h), F32), V((2, c, w), F32), V((2, a + b, h), F32), V((2, c, h), F32),
        V((2, a + b, h), F32), V((2, c, h), F32), V((a + b, h), F32), V((c, h), F32), V((r, h), F32),
        DMA((3,)), DMA((3,)), DMA, DMA, DMA,
        DMA((2,)), DMA((4,)), DMA((2, 3)), DMA((2, 3)), DMA((3,)), DMA((3,)), DMA((2,)), DMA((2,)), DMA((2,)), DMA((2,)),
        DMA, DMA((2, 4)), DMA, pltpu.SemaphoreType.REGULAR((11,)),
    ]


def solution(mesh):
    row_spec = P(('dz', 'dy', 'dx'), None)
    full_spec = P(None, None)

    def per_device(act_one, pre_one, act_two, pre_two, grad_out, w_in_two, w_out_one, w_out_two):
        dims = Dims(*grad_out.shape)
        any_spec = pl.BlockSpec(memory_space=pl.ANY)
        shards = pl.pallas_call(
            functools.partial(kernel, dims),
            out_shape=jax.ShapeDtypeStruct((4, dims.rows, dims.width), F32),
            in_specs=[any_spec] * 8,
            out_specs=any_spec,
            scratch_shapes=scratch(dims),
            compiler_params=pltpu.CompilerParams(collective_id=0, has_side_effects=True, vmem_limit_bytes=67043328),
        )(pre_two, pre_one, act_two, act_one, grad_out, w_in_two, w_out_one, w_out_two)
        across = jnp.transpose(shards, (1, 0, 2)).reshape(-1)
        return jnp.where(lax.axis_index('dx') % 2 == 0, shards.reshape(-1), across)

    return jax.shard_map(per_device, mesh=mesh, in_specs=(row_spec,) * 5 + (full_spec,) * 3, out_specs=P(('dx', 'dy', 'dz')), check_vma=False)
```

```python
import functools

import jax
import jax.numpy as jnp
from jax import lax
from jax.experimental import pallas as pl
from jax.experimental.pallas import tpu as pltpu
from jax.sharding import PartitionSpec as P

MESH = pl.DeviceIdType.MESH
F32 = jnp.float32
BF16 = jnp.bfloat16
N_CHUNK = 8
GRANULES = 2 * N_CHUNK
FIRST, LAG = 2, 2
ROOT = 0.7978845608028654
CUBE = 0.044715


def gelu_hidden(pre):
    square = pre * pre
    bend = jnp.tanh(pre * (ROOT + (ROOT * CUBE) * square))
    half = 0.5 * pre
    return half + half * bend


def gelu_slope(pre):
    square = pre * pre
    bend = jnp.tanh(pre * (ROOT + (ROOT * CUBE) * square))
    tail = ((1.0 - bend * bend) * pre) * ((1.5 * ROOT * CUBE) * square + 0.5 * ROOT)
    return (0.5 + 0.5 * bend) + tail


def dot_nn(left, right):
    return lax.dot_general(left, right, (((1,), (0,)), ((), ())), preferred_element_type=F32)


def dot_nt(left, right):
    return lax.dot_general(left, right, (((1,), (1,)), ((), ())), preferred_element_type=F32)


class Dims:
    def __init__(self, tokens, width):
        self.tokens = tokens
        self.micro = tokens // 2
        self.width = width
        self.hidden = 4 * width
        self.rows = width // 8
        self.tile = 2 * self.rows
        self.half = width // 2
        self.quarter = width // 4
        unit = self.rows // 16
        self.row_a = max(8, (unit * 5) // 8 * 8)
        self.row_c = 4 * unit
        self.row_b = self.rows - self.row_a - self.row_c
        self.block = min(256, self.micro)
        self.span = min(512, width)


def kernel(dims, z2, z1, x2, x1, dy, win2, wo1, wo2, out,
           gin, xt, acc, dz, zbuf, wbuf, winbuf, ht, stage, rcore,
           s1, r1a, r1b, r1c, s2a, s2b, s2c, r2a, r2b, r2c, s3ab, s3c, r3ab, r3c, s4ab, s4c, r4ab, r4c, fin,
           zsem, wsem, winsem, xsem, gsem,
           core_send, core_recv, send1, recv1, send2, recv2, send3, recv3, send4, recv4,
           fin_send, fin_recv, fin_local, credit):
    rows, tile, width, half, quarter = dims.rows, dims.tile, dims.width, dims.half, dims.quarter
    micro, tokens, block, span = dims.micro, dims.tokens, dims.block, dims.span
    row_a, row_b, row_c = dims.row_a, dims.row_b, dims.row_c
    row_ab = row_a + row_b
    lanes = 128
    iz, iy, ix = lax.axis_index('dz'), lax.axis_index('dy'), lax.axis_index('dx')
    px, core = ix // 2, ix % 2
    zhi, zlo = iz // 2, iz % 2
    to_core = (iz, iy, px * 2 + (1 - core))
    to_x = (iz, iy, (1 - px) * 2 + core)
    to_xc = (iz, iy, (1 - px) * 2 + (1 - core))
    to_y = (iz, 1 - iy, ix)
    to_za = (zhi * 2 + (1 - zlo), iy, ix)
    to_zb = ((1 - zhi) * 2 + zlo, iy, ix)
    keep_x = pl.ds(pl.multiple_of(px * quarter, min(quarter, lanes)), quarter)
    send_x = pl.ds(pl.multiple_of((1 - px) * quarter, min(quarter, lanes)), quarter)
    CORE, A1, B1, C1, A2, B2, C2, AB3, C3, AB4, C4 = range(11)

    barrier = pltpu.get_barrier_semaphore()
    for peer in (to_core, to_x, to_xc, to_y, to_za, to_zb):
        pl.semaphore_signal(barrier, inc=1, device_id=peer, device_id_type=MESH)

    def order(num):
        k, t = num // 8, num % 8
        b, i, g = k // 4, (k // 2) % 2, k % 2
        plain_s, plain_p = t // 4, t % 4
        first = jnp.logical_or(t == 0, jnp.logical_and(t % 2 == 1, t < 7))
        mixed_s = jnp.where(first, 0, 1)
        mixed_p = jnp.where(first, (t + 1) // 2, jnp.where(t == 7, 3, t // 2 - 1))
        s = jnp.where(g == 0, mixed_s, plain_s)
        p = jnp.where(g == 0, mixed_p, plain_p)
        return k, b, i, g, s, p

    def piece_start(num):
        k, b, i, g, s, p = order(num)
        j = 2 * i + jnp.where(s == 0, 1 - core, core)
        slot = num % 3

        def from_block(zref, wref):
            @pl.when(g == 0)
            def _():
                for h in range(2):
                    col = pl.multiple_of((dims.hidden // 8) * (2 * p + h) + rows * j, rows)
                    pltpu.make_async_copy(zref.at[:, pl.ds(col, rows)], zbuf.at[slot, :, pl.ds(h * rows, rows)], zsem.at[slot]).start()

            @pl.when(g == 1)
            def _():
                col = pl.multiple_of(width * j + tile * p, tile)
                pltpu.make_async_copy(zref.at[:, pl.ds(col, tile)], zbuf.at[slot], zsem.at[slot]).start()
                pltpu.make_async_copy(wref.at[pl.ds(col, tile), :], wbuf.at[slot], wsem.at[slot]).start()

        @pl.when(b == 0)
        def _():
            from_block(z2, wo2)

        @pl.when(b == 1)
        def _():
            from_block(z1, wo1)

    def piece_ahead(num):
        @pl.when(num + 2 < 8 * N_CHUNK)
        def _():
            piece_start(num + 2)

    def z_wait(num):
        pltpu.make_async_copy(z2.at[:, pl.ds(0, tile)], zbuf.at[num % 3], zsem.at[num % 3]).wait()

    def w_wait(num):
        pltpu.make_async_copy(wo2.at[pl.ds(0, tile), :], wbuf.at[num % 3], wsem.at[num % 3]).wait()

    def x_copy(xref):
        return pltpu.make_async_copy(xref, dz, xsem)

    def core_copy(p):
        return pltpu.make_async_remote_copy(stage.at[p % 2], rcore.at[p], core_send.at[p % 2], core_recv.at[p], device_id=to_core, device_id_type=MESH)

    def remote(src, dst, sends, recvs, peer):
        return pltpu.make_async_remote_copy(src, dst, sends, recvs, device_id=peer, device_id_type=MESH)

    def shift(q, part, size):
        return pl.ds(pl.multiple_of((q % 2) * half + part, min(quarter, lanes)), size)

    def phase1(q):
        slot, r = (q // 2) % 2, q % 4
        return (
            remote(s1.at[slot, :, :, :, pl.ds(0, row_a), shift(q, (1 - px) * quarter, quarter)], r1a.at[r], send1.at[r, 0], recv1.at[r, 0], to_x),
            remote(s1.at[slot, 1 - iy, :, :, pl.ds(row_a, row_b), shift(q, 0, half)], r1b.at[r], send1.at[r, 1], recv1.at[r, 1], to_y),
            remote(s1.at[slot, :, :, 1 - zlo, pl.ds(row_ab, row_c), shift(q, 0, half)], r1c.at[r], send1.at[r, 2], recv1.at[r, 2], to_za),
        )

    def phase1_early(q, p):
        slot, r = (q // 2) % 2, q % 4
        ty, tz = p // 2, p % 2
        remote(s1.at[slot, ty, tz, :, pl.ds(0, row_a), shift(q, (1 - px) * quarter, quarter)], r1a.at[r, ty, tz], send1.at[r, 0], recv1.at[r, 0], to_x).start()
        remote(s1.at[slot, ty, tz, 1 - zlo, pl.ds(row_ab, row_c), shift(q, 0, half)], r1c.at[r, ty, tz], send1.at[r, 2], recv1.at[r, 2], to_za).start()

        @pl.when(ty != iy)
        def _():
            remote(s1.at[slot, ty, tz, :, pl.ds(row_a, row_b), shift(q, 0, half)], r1b.at[r, tz], send1.at[r, 1], recv1.at[r, 1], to_y).start()

    def phase2(q):
        r, v = q % 4, q % 2
        return (
            remote(s2a.at[v, 1 - iy], r2a.at[r], send2.at[r, 0], recv2.at[r, 0], to_y),
            remote(s2b.at[v, :, :, :, send_x], r2b.at[r], send2.at[r, 1], recv2.at[r, 1], to_x),
            remote(s2c.at[v, :, 1 - zhi], r2c.at[r], send2.at[r, 2], recv2.at[r, 2], to_zb),
        )

    def phase3(q):
        r, v = q % 4, q % 2
        return (
            remote(s3ab.at[v, :, 1 - zlo], r3ab.at[r], send3.at[r, 0], recv3.at[r, 0], to_za),
            remote(s3c.at[v, :, :, send_x], r3c.at[r], send3.at[r, 1], recv3.at[r, 1], to_x),
        )

    def phase4(q):
        r, v = q % 4, q % 2
        return (
            remote(s4ab.at[v, 1 - zhi], r4ab.at[r], send4.at[r, 0], recv4.at[r, 0], to_zb),
            remote(s4c.at[v, 1 - iy], r4c.at[r], send4.at[r, 1], recv4.at[r, 1], to_y),
        )

    def grant(kind, peer, ok):
        @pl.when(ok)
        def _():
            pl.semaphore_signal(credit.at[kind], inc=1, device_id=peer, device_id_type=MESH)

    def claim(kind, ok):
        @pl.when(ok)
        def _():
            pl.semaphore_wait(credit.at[kind], 1)

    def out_place(q, n):
        i, h = (q // 4) % 2, q % 2
        j = 2 * i + core
        strip = (width // lanes // 2) * h + (width // lanes // 4) * px + n
        return (
            out.at[pl.ds(pl.multiple_of(j * rows, rows), rows), strip, :],
            out.reshape(rows, 4, width // lanes, lanes).at[:, j, strip, :],
        )

    def owner_of(q):
        return 2 * (q // 8) + (q // 2) % 2

    def fin_start(q):
        f = q % 2
        for g in range(2):
            @pl.when((q // 2) % 2 == g)
            def _():
                for n in range(quarter // lanes):
                    strip = fin.at[f, :, pl.ds(n * lanes, lanes)]
                    place = out_place(q, n)[g]

                    @pl.when(owner_of(q) == ix)
                    def _():
                        pltpu.make_async_copy(strip, place, fin_local.at[f]).start()

                    @pl.when(owner_of(q) != ix)
                    def _():
                        remote(strip, place, fin_send.at[f], fin_recv.at[(q // 4) % 2, q % 2, ix], (iz, iy, owner_of(q))).start()

    def fin_wait(q):
        f = q % 2

        @pl.when(owner_of(q) == ix)
        def _():
            pltpu.make_async_copy(fin.at[f], fin.at[f], fin_local.at[f]).wait()

        @pl.when(owner_of(q) != ix)
        def _():
            remote(fin.at[f], fin.at[f], fin_send.at[f], fin_recv.at[0, 0, ix], to_core).wait_send()

    def service(step):
        def stage_of(phase, act):
            q = step - (FIRST + LAG * (phase - 1))

            @pl.when(jnp.logical_and(q >= 0, q < GRANULES))
            def _():
                act(q, q % 4, q % 2, q < GRANULES - 4, q >= 4)

        def take4(q, r, v, more, later):
            ab, c = phase4(q)

            @pl.when(q >= 2)
            def _():
                fin_wait(q - 2)
            ab.wait()
            fin[v, 0:row_ab, :] = s4ab[v, zhi] + r4ab[r]
            grant(AB4, to_zb, more)
            c.wait()
            fin[v, row_ab:rows, :] = s4c[v, iy] + r4c[r]
            grant(C4, to_y, more)
            fin_start(q)

        def take3(q, r, v, more, later):
            ab, c = phase3(q)
            ab4, c4 = phase4(q)
            ab.wait()
            s4ab[v] = s3ab[v, :, zlo] + r3ab[r]
            grant(AB3, to_za, more)
            claim(AB4, later)
            ab4.start()
            c.wait()
            s4c[v] = s3c[v, :, :, keep_x] + r3c[r]
            grant(C3, to_x, more)
            claim(C4, later)
            c4.start()

        def take2(q, r, v, more, later):
            a, b, c = phase2(q)
            ab3, c3 = phase3(q)
            a.wait()
            s3ab[v, :, :, 0:row_a, :] = s2a[v, iy] + r2a[r]
            grant(A2, to_y, more)
            b.wait()
            s3ab[v, :, :, row_a:row_ab, :] = s2b[v, :, :, :, keep_x] + r2b[r]
            grant(B2, to_x, more)
            claim(AB3, later)
            ab3.start()
            c.wait()
            s3c[v] = s2c[v, :, zhi] + r2c[r]
            grant(C2, to_zb, more)
            claim(C3, later)
            c3.start()

        def take1(q, r, v, more, later):
            slot = (q // 2) % 2
            a, b, c = phase1(q)
            a2, b2, c2 = phase2(q)
            a.wait()
            s2a[v] = s1[slot, :, :, :, 0:row_a, shift(q, px * quarter, quarter)] + r1a[r]
            grant(A1, to_x, more)
            claim(A2, later)
            a2.start()
            b.wait()
            s2b[v] = s1[slot, iy, :, :, row_a:row_ab, shift(q, 0, half)] + r1b[r]
            grant(B1, to_y, more)
            claim(B2, later)
            b2.start()
            c.wait()
            s2c[v] = s1[slot, :, :, zlo, row_ab:rows, shift(q, 0, half)] + r1c[r]
            grant(C1, to_za, more)
            claim(C2, later)
            c2.start()

        stage_of(4, take4)
        stage_of(3, take3)
        stage_of(2, take2)
        stage_of(1, take1)

    def emit_tile(k, s, p, cols, value):
        @pl.when(s == 0)
        def _():
            stage[p % 2, :, cols] = value

        @pl.when(s == 1)
        def _():
            total = value + rcore[p, :, cols]
            s1[k % 2, p // 2, p % 2, 0, :, cols] = total[0:rows]
            s1[k % 2, p // 2, p % 2, 1, :, cols] = total[rows:tile]

    def tile_open(k, s, p):
        @pl.when(s == 0)
        def _():
            @pl.when(jnp.logical_or(k >= 1, p >= 2))
            def _():
                core_copy(p).wait_send()

        @pl.when(s == 1)
        def _():
            core_copy(p).wait_recv()

    def tile_close(k, s, p):
        @pl.when(s == 0)
        def _():
            claim(CORE, k >= 1)
            core_copy(p).start()

        @pl.when(s == 1)
        def _():
            grant(CORE, to_core, k < N_CHUNK - 1)

            @pl.when(k == 0)
            def _():
                for q in range(2):
                    phase1_early(q, p)

    def hidden_block(num, side, r):
        part = slice(r * block, (r + 1) * block)
        ht[side, :, part] = gelu_hidden(zbuf[num % 3, part, :].astype(F32)).astype(BF16).T

    def product(left, right, cols):
        value = None
        for m in range(2):
            part = slice(m * micro, (m + 1) * micro)
            term = dot_nn(left(part), right(part, cols)).astype(BF16).astype(F32)
            value = term if value is None else value + term
        return value

    n_block, n_span = tokens // block, width // span

    def half_out(step):
        @pl.when(step % 2 == 0)
        def _():
            z_wait(step * 4)
            for r in range(n_block):
                hidden_block(step * 4, 0, r)

        @pl.loop(0, 4)
        def _(t):
            num = step * 4 + t
            k, b, i, g, s, p = order(num)
            piece_ahead(num)
            more = num % 8 < 7

            @pl.when(more)
            def _():
                z_wait(num + 1)
            ahead = jnp.where(more, num + 1, num)
            side = num % 2
            tile_open(k, s, p)
            for n in range(n_span):
                cols = slice(n * span, (n + 1) * span)
                value = product(lambda part: ht[side, :, part], lambda part, c: gin[part, c], cols)
                for r in range(n * n_block // n_span, (n + 1) * n_block // n_span):
                    hidden_block(ahead, 1 - side, r)
                emit_tile(k, s, p, cols, value)
            tile_close(k, s, p)

    def half_in(step):
        k, s = step // 2, step % 2
        b, i = k // 4, (k // 2) % 2
        j = 2 * i + jnp.where(s == 0, 1 - core, core)

        @pl.when(b == 0)
        def _():
            pltpu.make_async_copy(win2.at[:, pl.ds(pl.multiple_of(width * j, width), width)], winbuf, winsem).start()

        @pl.loop(0, 4)
        def _(p):
            num = step * 4 + p
            piece_ahead(num)
            z_wait(num)
            w_wait(num)
            slot = num % 3
            where = pl.ds(pl.multiple_of(p * tile, tile), tile)
            for r in range(n_block):
                part = slice(r * block, (r + 1) * block)
                back = dot_nt(gin[part, :], wbuf[slot])
                dz[part, where] = (back * gelu_slope(zbuf[slot, part, :].astype(F32))).astype(BF16)

        @pl.loop(0, 4)
        def _(p):
            lines = pl.ds(pl.multiple_of(p * tile, tile), tile)
            tile_open(k, s, p)
            for n in range(n_span):
                cols = slice(n * span, (n + 1) * span)
                emit_tile(k, s, p, cols, product(lambda part: xt[lines, part], lambda part, c: dz[part, c], cols))
            tile_close(k, s, p)

    def pass_back():
        pltpu.make_async_copy(win2.at[:, pl.ds(0, width)], winbuf, winsem).wait()

        @pl.loop(0, width // tile)
        def _(n):
            lines = pl.ds(pl.multiple_of(n * tile, tile), tile)
            for m in range(2):
                part = slice(m * micro, (m + 1) * micro)
                acc[part, lines] += dot_nt(dz[part, :], winbuf[lines, :])

    piece_start(0)
    first = pltpu.make_async_copy(dy, gin, gsem)
    first.start()
    piece_start(1)
    x_copy(x2).start()
    first.wait()
    pl.semaphore_wait(barrier, 6)

    @pl.loop(0, GRANULES + FIRST + 3 * LAG)
    def _(step):
        k, g, s = step // 2, (step // 2) % 2, step % 2

        @pl.when(step == 2)
        def _():
            @pl.loop(0, n_block)
            def _(r):
                part = pl.ds(pl.multiple_of(r * block, block), block)
                acc[part, :] = gin[part, :].astype(F32)

        @pl.when(step == N_CHUNK)
        def _():
            x_copy(x1).start()

            @pl.loop(0, n_block)
            def _(r):
                part = pl.ds(pl.multiple_of(r * block, block), block)
                gin[part, :] = acc[part, :].astype(BF16)

        @pl.when(jnp.logical_or(step == 2, step == N_CHUNK + 2))
        def _():
            x_copy(x2).wait()

            @pl.loop(0, n_block)
            def _(r):
                part = pl.ds(pl.multiple_of(r * block, block), block)
                for c in range(width // tile):
                    xt[c * tile:(c + 1) * tile, part] = dz[part, c * tile:(c + 1) * tile].T

        @pl.when(step < GRANULES)
        def _():
            @pl.when(g == 0)
            def _():
                half_out(step)

            @pl.when(g == 1)
            def _():
                half_in(step)

            @pl.when(jnp.logical_and(s == 1, k >= 1))
            def _():
                for h in range(2):
                    claim(A1, k >= 2)
                    claim(B1, k >= 2)
                    claim(C1, k >= 2)
                    for copy in phase1(2 * k + h):
                        copy.start()

            @pl.when(jnp.logical_and(g == 1, k < N_CHUNK // 2))
            def _():
                pass_back()
        service(step)

    for p in range(2):
        core_copy(p).wait_send()
    for q in range(2):
        fin_wait(GRANULES - 2 + q)
    for i in range(2):
        for h in range(2):
            for d in range(4):
                @pl.when(ix != d)
                def _():
                    remote(fin.at[0], fin.at[0], fin_send.at[0], fin_recv.at[i, h, d], to_core).wait_recv()


def scratch(dims):
    t, w, r, h, q = dims.tokens, dims.width, dims.rows, dims.half, dims.quarter
    a, b, c = dims.row_a, dims.row_b, dims.row_c
    tile = dims.tile
    V, DMA = pltpu.VMEM, pltpu.SemaphoreType.DMA
    return [
        V((t, w), BF16), V((w, t), BF16), V((t, w), F32), V((t, w), BF16), V((3, t, tile), BF16), V((3, tile, w), BF16), V((w, w), BF16),
        V((2, tile, t), BF16), V((2, tile, w), F32), V((4, tile, w), F32),
        V((2, 2, 2, 2, r, w), F32), V((4, 2, 2, 2, a, q), F32), V((4, 2, 2, b, h), F32), V((4, 2, 2, c, h), F32),
        V((2, 2, 2, 2, a, q), F32), V((2, 2, 2, b, h), F32), V((2, 2, 2, c, h), F32),
        V((4, 2, 2, a, q), F32), V((4, 2, 2, b, q), F32), V((4, 2, c, h), F32),
        V((2, 2, 2, a + b, q), F32), V((2, 2, c, h), F32), V((4, 2, a + b, q), F32), V((4, 2, c, q), F32),
        V((2, 2, a + b, q), F32), V((2, 2, c, q), F32), V((4, a + b, q), F32), V((4, c, q), F32), V((2, r, q), F32),
        DMA((3,)), DMA((3,)), DMA, DMA, DMA,
        DMA((2,)), DMA((4,)), DMA((4, 3)), DMA((4, 3)), DMA((4, 3)), DMA((4, 3)), DMA((4, 2)), DMA((4, 2)), DMA((4, 2)), DMA((4, 2)),
        DMA((2,)), DMA((2, 2, 4)), DMA((2,)), pltpu.SemaphoreType.REGULAR((11,)),
    ]


def solution(mesh):
    row_spec = P(('dz', 'dy', 'dx'), None)
    full_spec = P(None, None)

    def per_device(act_one, pre_one, act_two, pre_two, grad_out, w_in_two, w_out_one, w_out_two):
        dims = Dims(*grad_out.shape)
        any_spec = pl.BlockSpec(memory_space=pl.ANY)
        shard = pl.pallas_call(
            functools.partial(kernel, dims),
            out_shape=jax.ShapeDtypeStruct((4 * dims.rows, dims.width // 128, 128), F32),
            in_specs=[any_spec] * 8,
            out_specs=any_spec,
            scratch_shapes=scratch(dims),
            compiler_params=pltpu.CompilerParams(collective_id=0, has_side_effects=True, vmem_limit_bytes=67043328),
        )(pre_two, pre_one, act_two, act_one, grad_out, w_in_two, w_out_one, w_out_two)
        return shard.reshape(-1)

    return jax.shard_map(per_device, mesh=mesh, in_specs=(row_spec,) * 5 + (full_spec,) * 3, out_specs=P(('dx', 'dy', 'dz')), check_vma=False)
```

```python
import functools

import jax
import jax.numpy as jnp
from jax import lax
from jax.experimental import pallas as pl
from jax.experimental.pallas import tpu as pltpu
from jax.sharding import PartitionSpec as P

MESH = pl.DeviceIdType.MESH
F32 = jnp.float32
BF16 = jnp.bfloat16
N_CHUNK = 8
GRANULES = 2 * N_CHUNK
TAKE = (
    (14, 16, 19, 20, 25, 28, 34, 41, 48, 49, 55, 56, 62, 64, 70, 72),
    (18, 20, 21, 23, 28, 30, 41, 49, 57, 58, 66, 67, 71, 74, 78, 79),
    (20, 23, 26, 30, 31, 38, 49, 57, 65, 69, 73, 77, 81, 84, 85, 88),
    (22, 27, 28, 32, 38, 48, 57, 68, 75, 76, 80, 82, 83, 86, 87, 89),
)
ROOT = 0.7978845608028654
CUBE = 0.044715


def gelu_hidden(pre):
    square = pre * pre
    bend = jnp.tanh(pre * (ROOT + (ROOT * CUBE) * square))
    half = 0.5 * pre
    return half + half * bend


def gelu_slope(pre):
    square = pre * pre
    bend = jnp.tanh(pre * (ROOT + (ROOT * CUBE) * square))
    tail = ((1.0 - bend * bend) * pre) * ((1.5 * ROOT * CUBE) * square + 0.5 * ROOT)
    return (0.5 + 0.5 * bend) + tail


def dot_nn(left, right):
    return lax.dot_general(left, right, (((1,), (0,)), ((), ())), preferred_element_type=F32)


def dot_nt(left, right):
    return lax.dot_general(left, right, (((1,), (1,)), ((), ())), preferred_element_type=F32)


class Dims:
    def __init__(self, tokens, width):
        self.tokens = tokens
        self.micro = tokens // 2
        self.width = width
        self.hidden = 4 * width
        self.rows = width // 8
        self.tile = 2 * self.rows
        self.half = width // 2
        self.quarter = width // 4
        unit = self.rows // 16
        self.row_a = max(8, (unit * 5) // 8 * 8)
        self.row_c = 4 * unit
        self.row_b = self.rows - self.row_a - self.row_c
        self.block = min(256, self.micro)
        self.span = min(512, width)


def kernel(dims, z2, z1, x2, x1, dy, win2, wo1, wo2, out,
           gin, xt, acc, dz, zbuf, wbuf, winbuf, ht, rcore,
           sums, r1a, r1b, r1c, s2a, s2b, s2c, r2a, r2b, r2c, s3ab, s3c, r3ab, r3c, s4ab, s4c, r4ab, r4c, fin,
           zsem, wsem, winsem, xsem, gsem,
           core_send, core_recv, send1, recv1, send2, recv2, send3, recv3, send4, recv4,
           fin_send, fin_recv, fin_local, credit):
    rows, tile, width, half, quarter = dims.rows, dims.tile, dims.width, dims.half, dims.quarter
    micro, tokens, block, span = dims.micro, dims.tokens, dims.block, dims.span
    row_a, row_b, row_c = dims.row_a, dims.row_b, dims.row_c
    row_ab = row_a + row_b
    lanes = 128
    iz, iy, ix = lax.axis_index('dz'), lax.axis_index('dy'), lax.axis_index('dx')
    px, core = ix // 2, ix % 2
    zhi, zlo = iz // 2, iz % 2
    to_core = (iz, iy, px * 2 + (1 - core))
    to_x = (iz, iy, (1 - px) * 2 + core)
    to_xc = (iz, iy, (1 - px) * 2 + (1 - core))
    to_y = (iz, 1 - iy, ix)
    to_za = (zhi * 2 + (1 - zlo), iy, ix)
    to_zb = ((1 - zhi) * 2 + zlo, iy, ix)
    keep_x = pl.ds(pl.multiple_of(px * quarter, min(quarter, lanes)), quarter)
    send_x = pl.ds(pl.multiple_of((1 - px) * quarter, min(quarter, lanes)), quarter)
    CORE, A1, B1, C1, A2, B2, C2, AB3, C3, AB4, C4 = range(11)

    barrier = pltpu.get_barrier_semaphore()
    for peer in (to_core, to_x, to_xc, to_y, to_za, to_zb):
        pl.semaphore_signal(barrier, inc=1, device_id=peer, device_id_type=MESH)

    def order(num):
        k, t = num // 8, num % 8
        b, g, i = k // 4, (k // 2) % 2, k % 2
        plain_s, plain_p = t // 4, t % 4
        first = jnp.logical_or(t == 0, jnp.logical_and(t % 2 == 1, t < 7))
        mixed_s = jnp.where(first, 0, 1)
        mixed_p = jnp.where(first, (t + 1) // 2, jnp.where(t == 7, 3, t // 2 - 1))
        s = jnp.where(g == 0, mixed_s, plain_s)
        p = jnp.where(g == 0, mixed_p, plain_p)
        return k, b, i, g, s, p

    def piece_start(num):
        k, b, i, g, s, p = order(num)
        j = 2 * i + jnp.where(s == 0, 1 - core, core)
        slot = num % 3

        def from_block(zref, wref, with_win):
            @pl.when(g == 0)
            def _():
                for h in range(2):
                    col = pl.multiple_of((dims.hidden // 8) * (2 * p + h) + rows * j, rows)
                    pltpu.make_async_copy(zref.at[:, pl.ds(col, rows)], zbuf.at[slot, :, pl.ds(h * rows, rows)], zsem.at[slot]).start()

            @pl.when(g == 1)
            def _():
                col = pl.multiple_of(width * j + tile * p, tile)
                pltpu.make_async_copy(zref.at[:, pl.ds(col, tile)], zbuf.at[slot], zsem.at[slot]).start()
                pltpu.make_async_copy(wref.at[pl.ds(col, tile), :], wbuf.at[slot], wsem.at[slot]).start()
                if with_win:
                    pltpu.make_async_copy(win2.at[:, pl.ds(col, tile)], winbuf.at[slot], winsem.at[slot]).start()

        @pl.when(b == 0)
        def _():
            from_block(z2, wo2, True)

        @pl.when(b == 1)
        def _():
            from_block(z1, wo1, False)

    def piece_ahead(num):
        @pl.when(num + 2 < 8 * N_CHUNK)
        def _():
            piece_start(num + 2)

    def z_wait(num):
        pltpu.make_async_copy(z2.at[:, pl.ds(0, tile)], zbuf.at[num % 3], zsem.at[num % 3]).wait()

    def w_wait(num):
        pltpu.make_async_copy(wo2.at[pl.ds(0, tile), :], wbuf.at[num % 3], wsem.at[num % 3]).wait()

    def win_wait(num):
        pltpu.make_async_copy(win2.at[:, pl.ds(0, tile)], winbuf.at[num % 3], winsem.at[num % 3]).wait()

    def x_copy(xref, c):
        return pltpu.make_async_copy(xref.at[:, pl.ds(c * tile, tile)], dz.at[c % 2], xsem.at[c % 2])

    def core_copy(p):
        return pltpu.make_async_remote_copy(sums.at[8 + p % 2], rcore.at[p], core_send.at[p % 2], core_recv.at[p], device_id=to_core, device_id_type=MESH)

    def remote(src, dst, sends, recvs, peer):
        return pltpu.make_async_remote_copy(src, dst, sends, recvs, device_id=peer, device_id_type=MESH)

    def shift(q, part, size):
        return pl.ds(pl.multiple_of((q % 2) * half + part, min(quarter, lanes)), size)

    def phase1(q):
        base, r = (q // 2) % 2 * 4, q % 4
        return (
            remote(sums.at[pl.ds(base, 4), :, pl.ds(0, row_a), shift(q, (1 - px) * quarter, quarter)], r1a.at[r], send1.at[r, 0], recv1.at[r, 0], to_x),
            remote(sums.at[pl.ds(base + 2 * (1 - iy), 2), :, pl.ds(row_a, row_b), shift(q, 0, half)], r1b.at[r], send1.at[r, 1], recv1.at[r, 1], to_y),
            remote(sums.at[pl.ds(base, 4), 1 - zlo, pl.ds(row_ab, row_c), shift(q, 0, half)], r1c.at[r], send1.at[r, 2], recv1.at[r, 2], to_za),
        )

    def phase1_early(q, p):
        base, r = (q // 2) % 2 * 4, q % 4
        remote(sums.at[base + p, :, pl.ds(0, row_a), shift(q, (1 - px) * quarter, quarter)], r1a.at[r, p], send1.at[r, 0], recv1.at[r, 0], to_x).start()
        remote(sums.at[base + p, 1 - zlo, pl.ds(row_ab, row_c), shift(q, 0, half)], r1c.at[r, p], send1.at[r, 2], recv1.at[r, 2], to_za).start()

        @pl.when(p // 2 != iy)
        def _():
            remote(sums.at[base + p, :, pl.ds(row_a, row_b), shift(q, 0, half)], r1b.at[r, p % 2], send1.at[r, 1], recv1.at[r, 1], to_y).start()

    def phase1_claim(q, now):
        for kind in (A1, B1, C1):
            claim(kind, jnp.logical_and(q >= 4, now))

    def phase2(q):
        r = v = q % 4
        return (
            remote(s2a.at[v, pl.ds(2 * (1 - iy), 2)], r2a.at[r], send2.at[r, 0], recv2.at[r, 0], to_y),
            remote(s2b.at[v, :, :, :, send_x], r2b.at[r], send2.at[r, 1], recv2.at[r, 1], to_x),
            remote(s2c.at[v, :, 1 - zhi], r2c.at[r], send2.at[r, 2], recv2.at[r, 2], to_zb),
        )

    def phase3(q):
        r = v = q % 4
        return (
            remote(s3ab.at[v, :, 1 - zlo], r3ab.at[r], send3.at[r, 0], recv3.at[r, 0], to_za),
            remote(s3c.at[v, :, :, send_x], r3c.at[r], send3.at[r, 1], recv3.at[r, 1], to_x),
        )

    def phase4(q):
        r = v = q % 4
        return (
            remote(s4ab.at[v, 1 - zhi], r4ab.at[r], send4.at[r, 0], recv4.at[r, 0], to_zb),
            remote(s4c.at[v, 1 - iy], r4c.at[r], send4.at[r, 1], recv4.at[r, 1], to_y),
        )

    def grant(kind, peer, ok):
        @pl.when(ok)
        def _():
            pl.semaphore_signal(credit.at[kind], inc=1, device_id=peer, device_id_type=MESH)

    def claim(kind, ok):
        @pl.when(ok)
        def _():
            pl.semaphore_wait(credit.at[kind], 1)

    def out_place(q, n):
        i, h = (q // 2) % 2, q % 2
        j = 2 * i + core
        strip = (width // lanes // 2) * h + (width // lanes // 4) * px + n
        return (
            out.at[pl.ds(pl.multiple_of(j * rows, rows), rows), strip, :],
            out.reshape(rows, 4, width // lanes, lanes).at[:, j, strip, :],
        )

    def owner_of(q):
        return q // 4

    def fin_start(q):
        f = q % 2
        for g in range(2):
            @pl.when((q // 4) % 2 == g)
            def _():
                for n in range(quarter // lanes):
                    strip = fin.at[f, :, pl.ds(n * lanes, lanes)]
                    place = out_place(q, n)[g]

                    @pl.when(owner_of(q) == ix)
                    def _():
                        pltpu.make_async_copy(strip, place, fin_local.at[f]).start()

                    @pl.when(owner_of(q) != ix)
                    def _():
                        remote(strip, place, fin_send.at[f], fin_recv.at[(q // 2) % 2, q % 2, ix], (iz, iy, owner_of(q))).start()

    def fin_wait(q):
        f = q % 2

        @pl.when(owner_of(q) == ix)
        def _():
            pltpu.make_async_copy(fin.at[f], fin.at[f], fin_local.at[f]).wait()

        @pl.when(owner_of(q) != ix)
        def _():
            remote(fin.at[f], fin.at[f], fin_send.at[f], fin_recv.at[0, 0, ix], to_core).wait_send()

    def service(num):
        def stage_of(phase, act):
            q, through = 0, 0
            for when in TAKE[phase - 1]:
                q = q + jnp.where(num > when, 1, 0)
                through = through + jnp.where(num >= when, 1, 0)

            @pl.when(through > q)
            def _():
                act(q, q % 4, q % 4, q < GRANULES - 4, q >= 4)

        def take4(q, r, v, more, later):
            ab, c = phase4(q)

            @pl.when(q >= 2)
            def _():
                fin_wait(q - 2)
            ab.wait()
            f = q % 2
            fin[f, 0:row_ab, :] = s4ab[v, zhi] + r4ab[r]
            grant(AB4, to_zb, more)
            c.wait()
            fin[f, row_ab:rows, :] = s4c[v, iy] + r4c[r]
            grant(C4, to_y, more)
            fin_start(q)

        def take3(q, r, v, more, later):
            ab, c = phase3(q)
            ab4, c4 = phase4(q)
            ab.wait()
            s4ab[v] = s3ab[v, :, zlo] + r3ab[r]
            grant(AB3, to_za, more)
            claim(AB4, later)
            ab4.start()
            c.wait()
            s4c[v] = s3c[v, :, :, keep_x] + r3c[r]
            grant(C3, to_x, more)
            claim(C4, later)
            c4.start()

        def take2(q, r, v, more, later):
            a, b, c = phase2(q)
            ab3, c3 = phase3(q)
            a.wait()
            s3ab[v, :, :, 0:row_a, :] = s2a[v, pl.ds(2 * iy, 2)] + r2a[r]
            grant(A2, to_y, more)
            b.wait()
            s3ab[v, :, :, row_a:row_ab, :] = s2b[v, :, :, :, keep_x] + r2b[r]
            grant(B2, to_x, more)
            claim(AB3, later)
            ab3.start()
            c.wait()
            s3c[v] = s2c[v, :, zhi] + r2c[r]
            grant(C2, to_zb, more)
            claim(C3, later)
            c3.start()

        def take1(q, r, v, more, later):
            base = (q // 2) % 2 * 4
            a, b, c = phase1(q)
            a2, b2, c2 = phase2(q)
            a.wait()
            s2a[v] = sums[pl.ds(base, 4), :, 0:row_a, shift(q, px * quarter, quarter)] + r1a[r]
            grant(A1, to_x, more)
            claim(A2, later)
            a2.start()
            b.wait()
            s2b[v] = sums[pl.ds(base + 2 * iy, 2), :, row_a:row_ab, shift(q, 0, half)] + r1b[r]
            grant(B1, to_y, more)
            claim(B2, later)
            b2.start()
            c.wait()
            s2c[v] = (sums[pl.ds(base, 4), zlo, row_ab:rows, shift(q, 0, half)] + r1c[r]).reshape(2, 2, row_c, half)
            grant(C1, to_za, more)
            claim(C2, later)
            c2.start()

        stage_of(4, take4)
        stage_of(3, take3)
        stage_of(2, take2)
        stage_of(1, take1)

    def emit(to, into, source, cols, value):
        for h in range(2):
            sums[to, h, :, into] = value[h * rows:(h + 1) * rows] + rcore[source, h, :, cols]

    def tile_open(k, s, p):
        @pl.when(s == 0)
        def _():
            @pl.when(jnp.logical_or(k >= 1, p >= 2))
            def _():
                core_copy(p).wait_send()

        @pl.when(s == 1)
        def _():
            core_copy(p).wait_recv()

    def tile_close(k, s, p):
        @pl.when(s == 0)
        def _():
            claim(CORE, k >= 1)
            core_copy(p).start()

        @pl.when(s == 1)
        def _():
            grant(CORE, to_core, k < N_CHUNK - 1)

    def hidden_block(num, side, r):
        part = slice(r * block, (r + 1) * block)
        ht[side, :, part] = gelu_hidden(zbuf[num % 3, part, :].astype(F32)).astype(BF16).T

    def slope_block(num, side, r):
        part = slice(r * block, (r + 1) * block)
        back = dot_nt(gin[part, :], wbuf[num % 3])
        dz[side, part, :] = (back * gelu_slope(zbuf[num % 3, part, :].astype(F32))).astype(BF16)

    def rounded(value):
        return value.astype(BF16).astype(F32)

    n_block, n_span = tokens // block, width // span
    micros = [slice(m * micro, (m + 1) * micro) for m in range(2)]

    def tile_out(num):
        k, b, i, g, s, p = order(num)

        @pl.when(num % 32 == 0)
        def _():
            z_wait(num)
            for r in range(n_block):
                hidden_block(num, 0, r)

        @pl.when(num == 0)
        def _():
            first.wait()
            pl.semaphore_wait(barrier, 6)
        piece_ahead(num)
        more = num % 16 < 15

        @pl.when(more)
        def _():
            z_wait(num + 1)
        ahead = jnp.where(more, num + 1, num)
        side = num % 2
        tile_open(k, s, p)
        to = jnp.where(s == 0, 8 + p % 2, k % 2 * 4 + p)
        source = jnp.where(s == 0, 4, p)
        for n in range(n_span):
            cols = slice(n * span, (n + 1) * span)
            value = rounded(dot_nn(ht[side, :, micros[0]], gin[micros[0], cols])) + rounded(dot_nn(ht[side, :, micros[1]], gin[micros[1], cols]))
            for r in range(n * n_block // n_span, (n + 1) * n_block // n_span):
                hidden_block(ahead, 1 - side, r)
            emit(to, cols, source, cols, value)
        tile_close(k, s, p)

        @pl.when(s == 1)
        def _():
            for h in range(2):
                phase1_claim(2 * k + h, p == 0)
                phase1_early(2 * k + h, p)

    def tile_in(num):
        k, b, i, g, s, p = order(num)

        @pl.when(num % 32 == 16)
        def _():
            z_wait(num)
            w_wait(num)
            for r in range(n_block):
                slope_block(num, 0, r)
        piece_ahead(num)
        more = num % 16 < 15

        @pl.when(more)
        def _():
            z_wait(num + 1)
            w_wait(num + 1)
        ahead = jnp.where(more, num + 1, num)
        side = num % 2
        tile_open(k, s, p)
        source = jnp.where(s == 0, 4, p)
        for r in range(4):
            lines = slice(r * tile, (r + 1) * tile)
            to = jnp.where(s == 0, 8 + p % 2, k % 2 * 4 + r)
            into = pl.ds(pl.multiple_of(jnp.where(s == 0, r, p) * tile, tile), tile)
            spread = [range(r * n_block // 4 + m * n_block // 8, r * n_block // 4 + (m + 1) * n_block // 8) for m in range(2)]
            value = rounded(dot_nn(xt[lines, micros[0]], dz[side, micros[0], :]))
            for e in spread[0]:
                slope_block(ahead, 1 - side, e)
            value = value + rounded(dot_nn(xt[lines, micros[1]], dz[side, micros[1], :]))
            for e in spread[1]:
                slope_block(ahead, 1 - side, e)
            emit(to, into, source, lines, value)
        tile_close(k, s, p)

        @pl.when(jnp.logical_and(s == 1, p % 2 == 1))
        def _():
            q = 2 * k + p // 2
            phase1_claim(q, True)
            for copy in phase1(q):
                copy.start()

        @pl.when(b == 0)
        def _():
            win_wait(num)
            for r in range(n_block):
                part = slice(r * block, (r + 1) * block)
                acc[part, :] += dot_nt(dz[side, part, :], winbuf[num % 3])

    piece_start(0)
    first = pltpu.make_async_copy(dy, gin, gsem)
    first.start()
    piece_start(1)
    for c in range(2):
        x_copy(x2, c).start()
    rcore[4] = jnp.zeros((2, rows, width), F32)

    def turn(xref):
        for c in range(4):
            x_copy(xref, c).wait()

            @pl.loop(0, n_block)
            def _(r):
                part = pl.ds(pl.multiple_of(r * block, block), block)
                xt[c * tile:(c + 1) * tile, part] = dz[c % 2, part, :].T
            if c < 2:
                x_copy(xref, c + 2).start()

    tiles = 8 * N_CHUNK

    @pl.loop(0, max(max(row) for row in TAKE) + 1)
    def _(num):
        @pl.when(num == tiles // 4)
        def _():
            @pl.loop(0, n_block)
            def _(r):
                part = pl.ds(pl.multiple_of(r * block, block), block)
                acc[part, :] = gin[part, :].astype(F32)
            turn(x2)

        @pl.when(num == tiles // 2)
        def _():
            for c in range(2):
                x_copy(x1, c).start()

            @pl.loop(0, n_block)
            def _(r):
                part = pl.ds(pl.multiple_of(r * block, block), block)
                gin[part, :] = acc[part, :].astype(BF16)

        @pl.when(num == 3 * tiles // 4)
        def _():
            turn(x1)

        @pl.when(jnp.logical_and(num < tiles, num % 32 < 16))
        def _():
            tile_out(num)

        @pl.when(jnp.logical_and(num < tiles, num % 32 >= 16))
        def _():
            tile_in(num)
        service(num)

    for p in range(2):
        core_copy(p).wait_send()
    for q in range(2):
        fin_wait(GRANULES - 2 + q)
    for i in range(2):
        for h in range(2):
            for d in range(4):
                @pl.when(ix != d)
                def _():
                    remote(fin.at[0], fin.at[0], fin_send.at[0], fin_recv.at[i, h, d], to_core).wait_recv()


def scratch(dims):
    t, w, r, h, q = dims.tokens, dims.width, dims.rows, dims.half, dims.quarter
    a, b, c = dims.row_a, dims.row_b, dims.row_c
    tile = dims.tile
    V, DMA = pltpu.VMEM, pltpu.SemaphoreType.DMA
    return [
        V((t, w), BF16), V((w, t), BF16), V((t, w), F32), V((2, t, tile), BF16), V((3, t, tile), BF16), V((3, tile, w), BF16), V((3, w, tile), BF16),
        V((2, tile, t), BF16), V((5, 2, r, w), F32),
        V((10, 2, r, w), F32), V((4, 4, 2, a, q), F32), V((4, 2, 2, b, h), F32), V((4, 4, c, h), F32),
        V((4, 4, 2, a, q), F32), V((4, 2, 2, b, h), F32), V((4, 2, 2, c, h), F32),
        V((4, 2, 2, a, q), F32), V((4, 2, 2, b, q), F32), V((4, 2, c, h), F32),
        V((4, 2, 2, a + b, q), F32), V((4, 2, c, h), F32), V((4, 2, a + b, q), F32), V((4, 2, c, q), F32),
        V((4, 2, a + b, q), F32), V((4, 2, c, q), F32), V((4, a + b, q), F32), V((4, c, q), F32), V((2, r, q), F32),
        DMA((3,)), DMA((3,)), DMA((3,)), DMA((2,)), DMA,
        DMA((2,)), DMA((4,)), DMA((4, 3)), DMA((4, 3)), DMA((4, 3)), DMA((4, 3)), DMA((4, 2)), DMA((4, 2)), DMA((4, 2)), DMA((4, 2)),
        DMA((2,)), DMA((2, 2, 4)), DMA((2,)), pltpu.SemaphoreType.REGULAR((11,)),
    ]


def solution(mesh):
    row_spec = P(('dz', 'dy', 'dx'), None)
    full_spec = P(None, None)

    def per_device(act_one, pre_one, act_two, pre_two, grad_out, w_in_two, w_out_one, w_out_two):
        dims = Dims(*grad_out.shape)
        any_spec = pl.BlockSpec(memory_space=pl.ANY)
        shard = pl.pallas_call(
            functools.partial(kernel, dims),
            out_shape=jax.ShapeDtypeStruct((4 * dims.rows, dims.width // 128, 128), F32),
            in_specs=[any_spec] * 8,
            out_specs=any_spec,
            scratch_shapes=scratch(dims),
            compiler_params=pltpu.CompilerParams(collective_id=0, has_side_effects=True, vmem_limit_bytes=67043328),
        )(pre_two, pre_one, act_two, act_one, grad_out, w_in_two, w_out_one, w_out_two)
        return shard.reshape(-1)

    return jax.shard_map(per_device, mesh=mesh, in_specs=(row_spec,) * 5 + (full_spec,) * 3, out_specs=P(('dx', 'dy', 'dz')), check_vma=False)
```

```python
import functools

import jax
import jax.numpy as jnp
from jax import lax
from jax.experimental import pallas as pl
from jax.experimental.pallas import tpu as pltpu
from jax.sharding import PartitionSpec as P

MESH = pl.DeviceIdType.MESH
F32 = jnp.float32
BF16 = jnp.bfloat16
N_CHUNK = 8
GRANULES = 2 * N_CHUNK
FIN_SLOTS = 8
TAKE = (
    (14, 16, 19, 21, 24, 27, 32, 41, 48, 49, 54, 58, 60, 68, 69, 70),
    (18, 20, 23, 26, 27, 30, 48, 49, 56, 59, 64, 69, 71, 72, 77, 80),
    (22, 27, 31, 37, 47, 50, 59, 65, 67, 70, 74, 76, 79, 81, 83, 85),
    (26, 40, 48, 61, 63, 66, 73, 75, 78, 79, 81, 82, 84, 86, 87, 88),
)
STEPS = TAKE + (tuple(TAKE[3][-1] + when for when in (-1, 0, 1, 2)),)
ROOT = 0.7978845608028654
CUBE = 0.044715


def gelu_hidden(pre):
    square = pre * pre
    bend = jnp.tanh(pre * (ROOT + (ROOT * CUBE) * square))
    half = 0.5 * pre
    return half + half * bend


def gelu_slope(pre):
    square = pre * pre
    bend = jnp.tanh(pre * (ROOT + (ROOT * CUBE) * square))
    tail = ((1.0 - bend * bend) * pre) * ((1.5 * ROOT * CUBE) * square + 0.5 * ROOT)
    return (0.5 + 0.5 * bend) + tail


def dot_nn(left, right):
    return lax.dot_general(left, right, (((1,), (0,)), ((), ())), preferred_element_type=F32)


def dot_nt(left, right):
    return lax.dot_general(left, right, (((1,), (1,)), ((), ())), preferred_element_type=F32)


class Dims:
    def __init__(self, tokens, width):
        self.tokens = tokens
        self.micro = tokens // 2
        self.width = width
        self.hidden = 4 * width
        self.rows = width // 8
        self.tile = 2 * self.rows
        self.half = width // 2
        self.quarter = width // 4
        unit = self.rows // 16
        self.row_a = max(8, (unit * 5) // 8 * 8)
        self.row_c = 4 * unit
        self.row_b = self.rows - self.row_a - self.row_c
        self.block = min(256, self.micro)
        self.span = min(512, width)


def kernel(dims, z2, z1, x2, x1, dy, win2, wo1, wo2, out,
           gin, xt, acc, dz, zbuf, wbuf, winbuf, ht, rcore,
           sums, r1a, r1b, r1c, s2a, s2b, s2c, r2a, r2b, r2c, s3ab, s3c, r3ab, r3c, s4ab, s4c, r4ab, r4c, fin, shard,
           zsem, wsem, winsem, xsem, gsem,
           core_send, core_recv, send1, recv1, send2, recv2, send3, recv3, send4, recv4,
           fin_send, fin_recv, fin_local, credit):
    rows, tile, width, half, quarter = dims.rows, dims.tile, dims.width, dims.half, dims.quarter
    micro, tokens, block, span = dims.micro, dims.tokens, dims.block, dims.span
    row_a, row_b, row_c = dims.row_a, dims.row_b, dims.row_c
    row_ab = row_a + row_b
    lanes = 128
    iz, iy, ix = lax.axis_index('dz'), lax.axis_index('dy'), lax.axis_index('dx')
    px, core = ix // 2, ix % 2
    zhi, zlo = iz // 2, iz % 2
    to_core = (iz, iy, px * 2 + (1 - core))
    to_x = (iz, iy, (1 - px) * 2 + core)
    to_xc = (iz, iy, (1 - px) * 2 + (1 - core))
    to_y = (iz, 1 - iy, ix)
    to_za = (zhi * 2 + (1 - zlo), iy, ix)
    to_zb = ((1 - zhi) * 2 + zlo, iy, ix)
    keep_x = pl.ds(pl.multiple_of(px * quarter, min(quarter, lanes)), quarter)
    send_x = pl.ds(pl.multiple_of((1 - px) * quarter, min(quarter, lanes)), quarter)
    CORE, A1, B1, C1, A2, B2, C2, AB3, C3, AB4, C4 = range(11)

    barrier = pltpu.get_barrier_semaphore()
    for peer in (to_core, to_x, to_xc, to_y, to_za, to_zb):
        pl.semaphore_signal(barrier, inc=1, device_id=peer, device_id_type=MESH)

    def order(num):
        k, t = num // 8, num % 8
        b, g, i = k // 4, (k // 2) % 2, k % 2
        plain_s, plain_p = t // 4, t % 4
        first = jnp.logical_or(t == 0, jnp.logical_and(t % 2 == 1, t < 7))
        mixed_s = jnp.where(first, 0, 1)
        mixed_p = jnp.where(first, (t + 1) // 2, jnp.where(t == 7, 3, t // 2 - 1))
        s = jnp.where(g == 0, mixed_s, plain_s)
        p = jnp.where(g == 0, mixed_p, plain_p)
        return k, b, i, g, s, p

    def piece_start(num):
        k, b, i, g, s, p = order(num)
        j = 2 * i + jnp.where(s == 0, 1 - core, core)
        slot = num % 3

        def from_block(zref, wref, with_win):
            @pl.when(g == 0)
            def _():
                for h in range(2):
                    col = pl.multiple_of((dims.hidden // 8) * (2 * p + h) + rows * j, rows)
                    pltpu.make_async_copy(zref.at[:, pl.ds(col, rows)], zbuf.at[slot, :, pl.ds(h * rows, rows)], zsem.at[slot]).start()

            @pl.when(g == 1)
            def _():
                col = pl.multiple_of(width * j + tile * p, tile)
                pltpu.make_async_copy(zref.at[:, pl.ds(col, tile)], zbuf.at[slot], zsem.at[slot]).start()
                pltpu.make_async_copy(wref.at[pl.ds(col, tile), :], wbuf.at[slot], wsem.at[slot]).start()
                if with_win:
                    pltpu.make_async_copy(win2.at[:, pl.ds(col, tile)], winbuf.at[slot], winsem.at[slot]).start()

        @pl.when(b == 0)
        def _():
            from_block(z2, wo2, True)

        @pl.when(b == 1)
        def _():
            from_block(z1, wo1, False)

    def piece_ahead(num):
        @pl.when(num + 2 < 8 * N_CHUNK)
        def _():
            piece_start(num + 2)

    def z_wait(num):
        pltpu.make_async_copy(z2.at[:, pl.ds(0, tile)], zbuf.at[num % 3], zsem.at[num % 3]).wait()

    def w_wait(num):
        pltpu.make_async_copy(wo2.at[pl.ds(0, tile), :], wbuf.at[num % 3], wsem.at[num % 3]).wait()

    def win_wait(num):
        pltpu.make_async_copy(win2.at[:, pl.ds(0, tile)], winbuf.at[num % 3], winsem.at[num % 3]).wait()

    def x_copy(xref, c):
        return pltpu.make_async_copy(xref.at[:, pl.ds(c * tile, tile)], dz.at[c % 2], xsem.at[c % 2])

    def core_copy(p):
        return pltpu.make_async_remote_copy(sums.at[8 + p % 2], rcore.at[p], core_send.at[p % 2], core_recv.at[p], device_id=to_core, device_id_type=MESH)

    def remote(src, dst, sends, recvs, peer):
        return pltpu.make_async_remote_copy(src, dst, sends, recvs, device_id=peer, device_id_type=MESH)

    def shift(q, part, size):
        return pl.ds(pl.multiple_of((q % 2) * half + part, min(quarter, lanes)), size)

    def phase1(q):
        base, r = (q // 2) % 2 * 4, q % 4
        return (
            remote(sums.at[pl.ds(base, 4), :, pl.ds(0, row_a), shift(q, (1 - px) * quarter, quarter)], r1a.at[r], send1.at[r, 0], recv1.at[r, 0], to_x),
            remote(sums.at[pl.ds(base + 2 * (1 - iy), 2), :, pl.ds(row_a, row_b), shift(q, 0, half)], r1b.at[r], send1.at[r, 1], recv1.at[r, 1], to_y),
            remote(sums.at[pl.ds(base, 4), 1 - zlo, pl.ds(row_ab, row_c), shift(q, 0, half)], r1c.at[r], send1.at[r, 2], recv1.at[r, 2], to_za),
        )

    def phase1_early(q, p):
        base, r = (q // 2) % 2 * 4, q % 4
        remote(sums.at[base + p, :, pl.ds(0, row_a), shift(q, (1 - px) * quarter, quarter)], r1a.at[r, p], send1.at[r, 0], recv1.at[r, 0], to_x).start()
        remote(sums.at[base + p, 1 - zlo, pl.ds(row_ab, row_c), shift(q, 0, half)], r1c.at[r, p], send1.at[r, 2], recv1.at[r, 2], to_za).start()

        @pl.when(p // 2 != iy)
        def _():
            remote(sums.at[base + p, :, pl.ds(row_a, row_b), shift(q, 0, half)], r1b.at[r, p % 2], send1.at[r, 1], recv1.at[r, 1], to_y).start()

    def phase1_claim(q, now):
        for kind in (A1, B1, C1):
            claim(kind, jnp.logical_and(q >= 4, now))

    def phase2(q):
        r = v = q % 4
        return (
            remote(s2a.at[v, pl.ds(2 * (1 - iy), 2)], r2a.at[r], send2.at[r, 0], recv2.at[r, 0], to_y),
            remote(s2b.at[v, :, :, :, send_x], r2b.at[r], send2.at[r, 1], recv2.at[r, 1], to_x),
            remote(s2c.at[v, :, 1 - zhi], r2c.at[r], send2.at[r, 2], recv2.at[r, 2], to_zb),
        )

    def phase3(q):
        r = v = q % 4
        return (
            remote(s3ab.at[v, :, 1 - zlo], r3ab.at[r], send3.at[r, 0], recv3.at[r, 0], to_za),
            remote(s3c.at[v, :, :, send_x], r3c.at[r], send3.at[r, 1], recv3.at[r, 1], to_x),
        )

    def phase4(q):
        r = v = q % 4
        return (
            remote(s4ab.at[v, 1 - zhi], r4ab.at[r], send4.at[r, 0], recv4.at[r, 0], to_zb),
            remote(s4c.at[v, 1 - iy], r4c.at[r], send4.at[r, 1], recv4.at[r, 1], to_y),
        )

    def grant(kind, peer, ok):
        @pl.when(ok)
        def _():
            pl.semaphore_signal(credit.at[kind], inc=1, device_id=peer, device_id_type=MESH)

    def claim(kind, ok):
        @pl.when(ok)
        def _():
            pl.semaphore_wait(credit.at[kind], 1)

    def shard_place(q):
        i, h = (q // 2) % 2, q % 2
        return 2 * i + core, pl.ds(pl.multiple_of(half * h + quarter * px, lanes), quarter)

    def owner_of(q):
        return q // 4

    def fin_start(q):
        f = q % FIN_SLOTS
        j, cols = shard_place(q)

        @pl.when(owner_of(q) == ix)
        def _():
            shard[j, :, cols] = fin[f]

        @pl.when(owner_of(q) != ix)
        def _():
            remote(fin.at[f], shard.at[j, :, cols], fin_send.at[f], fin_recv.at[(q // 2) % 2, q % 2, ix], (iz, iy, owner_of(q))).start()

    def fin_wait(q):
        f = q % FIN_SLOTS

        @pl.when(owner_of(q) != ix)
        def _():
            remote(fin.at[f], fin.at[f], fin_send.at[f], fin_recv.at[0, 0, ix], to_core).wait_send()

    def part_out(q):
        i, h = (q // 2) % 2, q % 2
        for d in range(4):
            @pl.when(ix != d)
            def _():
                remote(fin.at[0], fin.at[0], fin_send.at[0], fin_recv.at[i, h, d], to_core).wait_recv()
        for g in range(2):
            @pl.when(core == g)
            def _():
                for c in range(2):
                    j = 2 * i + c
                    for n in range(half // lanes):
                        strip = (half // lanes) * h + n
                        if g == 0:
                            place = out.at[pl.ds(pl.multiple_of(j * rows, rows), rows), strip, :]
                        else:
                            place = out.reshape(rows, 4, width // lanes, lanes).at[:, j, strip, :]
                        pltpu.make_async_copy(shard.at[j, :, pl.ds(pl.multiple_of(strip * lanes, lanes), lanes)], place, fin_local).start()

    def service(num):
        def stage_of(phase, act):
            q, through = 0, 0
            for when in STEPS[phase - 1]:
                q = q + jnp.where(num > when, 1, 0)
                through = through + jnp.where(num >= when, 1, 0)

            @pl.when(through > q)
            def _():
                act(q, q % 4, q % 4, q < GRANULES - 4, q >= 4)

        def take4(q, r, v, more, later):
            ab, c = phase4(q)

            @pl.when(q >= FIN_SLOTS)
            def _():
                fin_wait(q - FIN_SLOTS)
            ab.wait()
            f = q % FIN_SLOTS
            fin[f, 0:row_ab, :] = s4ab[v, zhi] + r4ab[r]
            grant(AB4, to_zb, more)
            c.wait()
            fin[f, row_ab:rows, :] = s4c[v, iy] + r4c[r]
            grant(C4, to_y, more)
            fin_start(q)

        def take3(q, r, v, more, later):
            ab, c = phase3(q)
            ab4, c4 = phase4(q)
            ab.wait()
            s4ab[v] = s3ab[v, :, zlo] + r3ab[r]
            grant(AB3, to_za, more)
            claim(AB4, later)
            ab4.start()
            c.wait()
            s4c[v] = s3c[v, :, :, keep_x] + r3c[r]
            grant(C3, to_x, more)
            claim(C4, later)
            c4.start()

        def take2(q, r, v, more, later):
            a, b, c = phase2(q)
            ab3, c3 = phase3(q)
            a.wait()
            s3ab[v, :, :, 0:row_a, :] = s2a[v, pl.ds(2 * iy, 2)] + r2a[r]
            grant(A2, to_y, more)
            b.wait()
            s3ab[v, :, :, row_a:row_ab, :] = s2b[v, :, :, :, keep_x] + r2b[r]
            grant(B2, to_x, more)
            claim(AB3, later)
            ab3.start()
            c.wait()
            s3c[v] = s2c[v, :, zhi] + r2c[r]
            grant(C2, to_zb, more)
            claim(C3, later)
            c3.start()

        def take1(q, r, v, more, later):
            base = (q // 2) % 2 * 4
            a, b, c = phase1(q)
            a2, b2, c2 = phase2(q)
            a.wait()
            s2a[v] = sums[pl.ds(base, 4), :, 0:row_a, shift(q, px * quarter, quarter)] + r1a[r]
            grant(A1, to_x, more)
            claim(A2, later)
            a2.start()
            b.wait()
            s2b[v] = sums[pl.ds(base + 2 * iy, 2), :, row_a:row_ab, shift(q, 0, half)] + r1b[r]
            grant(B1, to_y, more)
            claim(B2, later)
            b2.start()
            c.wait()
            s2c[v] = (sums[pl.ds(base, 4), zlo, row_ab:rows, shift(q, 0, half)] + r1c[r]).reshape(2, 2, row_c, half)
            grant(C1, to_za, more)
            claim(C2, later)
            c2.start()

        stage_of(4, take4)
        stage_of(3, take3)
        stage_of(2, take2)
        stage_of(1, take1)

        def part(q, r, v, more, later):
            part_out(q)
        stage_of(5, part)

    def emit(to, into, source, cols, value):
        for h in range(2):
            sums[to, h, :, into] = value[h * rows:(h + 1) * rows] + rcore[source, h, :, cols]

    def tile_open(k, s, p):
        @pl.when(s == 0)
        def _():
            @pl.when(jnp.logical_or(k >= 1, p >= 2))
            def _():
                core_copy(p).wait_send()

        @pl.when(s == 1)
        def _():
            core_copy(p).wait_recv()

    def tile_close(k, s, p):
        @pl.when(s == 0)
        def _():
            claim(CORE, k >= 1)
            core_copy(p).start()

        @pl.when(s == 1)
        def _():
            grant(CORE, to_core, k < N_CHUNK - 1)

    def hidden_block(num, side, r):
        part = slice(r * block, (r + 1) * block)
        ht[side, :, part] = gelu_hidden(zbuf[num % 3, part, :].astype(F32)).astype(BF16).T

    def slope_block(num, side, r):
        part = slice(r * block, (r + 1) * block)
        back = dot_nt(gin[part, :], wbuf[num % 3])
        dz[side, part, :] = (back * gelu_slope(zbuf[num % 3, part, :].astype(F32))).astype(BF16)

    def rounded(value):
        return value.astype(BF16).astype(F32)

    n_block, n_span = tokens // block, width // span
    micros = [slice(m * micro, (m + 1) * micro) for m in range(2)]

    def tile_out(num):
        k, b, i, g, s, p = order(num)

        @pl.when(num % 32 == 0)
        def _():
            z_wait(num)
            for r in range(n_block):
                hidden_block(num, 0, r)

        @pl.when(num == 0)
        def _():
            first.wait()
            pl.semaphore_wait(barrier, 6)
        piece_ahead(num)
        more = num % 16 < 15

        @pl.when(more)
        def _():
            z_wait(num + 1)
        ahead = jnp.where(more, num + 1, num)
        side = num % 2
        tile_open(k, s, p)
        to = jnp.where(s == 0, 8 + p % 2, k % 2 * 4 + p)
        source = jnp.where(s == 0, 4, p)
        for n in range(n_span):
            cols = slice(n * span, (n + 1) * span)
            value = rounded(dot_nn(ht[side, :, micros[0]], gin[micros[0], cols])) + rounded(dot_nn(ht[side, :, micros[1]], gin[micros[1], cols]))
            for r in range(n * n_block // n_span, (n + 1) * n_block // n_span):
                hidden_block(ahead, 1 - side, r)
            emit(to, cols, source, cols, value)
        tile_close(k, s, p)

        @pl.when(s == 1)
        def _():
            for h in range(2):
                phase1_claim(2 * k + h, p == 0)
                phase1_early(2 * k + h, p)

    def tile_in(num):
        k, b, i, g, s, p = order(num)

        @pl.when(num % 32 == 16)
        def _():
            z_wait(num)
            w_wait(num)
            for r in range(n_block):
                slope_block(num, 0, r)
        piece_ahead(num)
        more = num % 16 < 15

        @pl.when(more)
        def _():
            z_wait(num + 1)
            w_wait(num + 1)
        ahead = jnp.where(more, num + 1, num)
        side = num % 2
        tile_open(k, s, p)
        source = jnp.where(s == 0, 4, p)
        for r in range(4):
            lines = slice(r * tile, (r + 1) * tile)
            to = jnp.where(s == 0, 8 + p % 2, k % 2 * 4 + r)
            into = pl.ds(pl.multiple_of(jnp.where(s == 0, r, p) * tile, tile), tile)
            spread = [range(r * n_block // 4 + m * n_block // 8, r * n_block // 4 + (m + 1) * n_block // 8) for m in range(2)]
            value = rounded(dot_nn(xt[lines, micros[0]], dz[side, micros[0], :]))
            for e in spread[0]:
                slope_block(ahead, 1 - side, e)
            value = value + rounded(dot_nn(xt[lines, micros[1]], dz[side, micros[1], :]))
            for e in spread[1]:
                slope_block(ahead, 1 - side, e)
            emit(to, into, source, lines, value)
        tile_close(k, s, p)

        @pl.when(jnp.logical_and(s == 1, p % 2 == 1))
        def _():
            q = 2 * k + p // 2
            phase1_claim(q, True)
            for copy in phase1(q):
                copy.start()

        @pl.when(b == 0)
        def _():
            win_wait(num)
            for r in range(n_block):
                part = slice(r * block, (r + 1) * block)
                acc[part, :] += dot_nt(dz[side, part, :], winbuf[num % 3])

    piece_start(0)
    first = pltpu.make_async_copy(dy, gin, gsem)
    first.start()
    piece_start(1)
    for c in range(2):
        x_copy(x2, c).start()
    rcore[4] = jnp.zeros((2, rows, width), F32)

    def turn(xref):
        for c in range(4):
            x_copy(xref, c).wait()

            @pl.loop(0, n_block)
            def _(r):
                part = pl.ds(pl.multiple_of(r * block, block), block)
                xt[c * tile:(c + 1) * tile, part] = dz[c % 2, part, :].T
            if c < 2:
                x_copy(xref, c + 2).start()

    tiles = 8 * N_CHUNK

    @pl.loop(0, max(max(row) for row in STEPS) + 1)
    def _(num):
        @pl.when(num == tiles // 4)
        def _():
            @pl.loop(0, n_block)
            def _(r):
                part = pl.ds(pl.multiple_of(r * block, block), block)
                acc[part, :] = gin[part, :].astype(F32)
            turn(x2)

        @pl.when(num == tiles // 2)
        def _():
            for c in range(2):
                x_copy(x1, c).start()

            @pl.loop(0, n_block)
            def _(r):
                part = pl.ds(pl.multiple_of(r * block, block), block)
                gin[part, :] = acc[part, :].astype(BF16)

        @pl.when(num == 3 * tiles // 4)
        def _():
            turn(x1)

        @pl.when(jnp.logical_and(num < tiles, num % 32 < 16))
        def _():
            tile_out(num)

        @pl.when(jnp.logical_and(num < tiles, num % 32 >= 16))
        def _():
            tile_in(num)
        service(num)

    for p in range(2):
        core_copy(p).wait_send()
    pltpu.make_async_copy(out.at[pl.ds(0, 4 * rows)], out.at[pl.ds(0, 4 * rows)], fin_local).wait()
    for q in range(FIN_SLOTS):
        fin_wait(GRANULES - FIN_SLOTS + q)


def scratch(dims):
    t, w, r, h, q = dims.tokens, dims.width, dims.rows, dims.half, dims.quarter
    a, b, c = dims.row_a, dims.row_b, dims.row_c
    tile = dims.tile
    V, DMA = pltpu.VMEM, pltpu.SemaphoreType.DMA
    return [
        V((t, w), BF16), V((w, t), BF16), V((t, w), F32), V((2, t, tile), BF16), V((3, t, tile), BF16), V((3, tile, w), BF16), V((3, w, tile), BF16),
        V((2, tile, t), BF16), V((5, 2, r, w), F32),
        V((10, 2, r, w), F32), V((4, 4, 2, a, q), F32), V((4, 2, 2, b, h), F32), V((4, 4, c, h), F32),
        V((4, 4, 2, a, q), F32), V((4, 2, 2, b, h), F32), V((4, 2, 2, c, h), F32),
        V((4, 2, 2, a, q), F32), V((4, 2, 2, b, q), F32), V((4, 2, c, h), F32),
        V((4, 2, 2, a + b, q), F32), V((4, 2, c, h), F32), V((4, 2, a + b, q), F32), V((4, 2, c, q), F32),
        V((4, 2, a + b, q), F32), V((4, 2, c, q), F32), V((4, a + b, q), F32), V((4, c, q), F32), V((FIN_SLOTS, r, q), F32), V((4, r, w), F32),
        DMA((3,)), DMA((3,)), DMA((3,)), DMA((2,)), DMA,
        DMA((2,)), DMA((4,)), DMA((4, 3)), DMA((4, 3)), DMA((4, 3)), DMA((4, 3)), DMA((4, 2)), DMA((4, 2)), DMA((4, 2)), DMA((4, 2)),
        DMA((FIN_SLOTS,)), DMA((2, 2, 4)), DMA, pltpu.SemaphoreType.REGULAR((11,)),
    ]


def solution(mesh):
    row_spec = P(('dz', 'dy', 'dx'), None)
    full_spec = P(None, None)

    def per_device(act_one, pre_one, act_two, pre_two, grad_out, w_in_two, w_out_one, w_out_two):
        dims = Dims(*grad_out.shape)
        any_spec = pl.BlockSpec(memory_space=pl.ANY)
        shard = pl.pallas_call(
            functools.partial(kernel, dims),
            out_shape=jax.ShapeDtypeStruct((4 * dims.rows, dims.width // 128, 128), F32),
            in_specs=[any_spec] * 8,
            out_specs=any_spec,
            scratch_shapes=scratch(dims),
            compiler_params=pltpu.CompilerParams(collective_id=0, has_side_effects=True, vmem_limit_bytes=67043328),
        )(pre_two, pre_one, act_two, act_one, grad_out, w_in_two, w_out_one, w_out_two)
        return shard.reshape(-1)

    return jax.shard_map(per_device, mesh=mesh, in_specs=(row_spec,) * 5 + (full_spec,) * 3, out_specs=P(('dx', 'dy', 'dz')), check_vma=False)
```

```python
import functools

import jax
import jax.numpy as jnp
from jax import lax
from jax.experimental import pallas as pl
from jax.experimental.pallas import tpu as pltpu
from jax.sharding import PartitionSpec as P

MESH = pl.DeviceIdType.MESH
F32 = jnp.float32
BF16 = jnp.bfloat16
N_CHUNK = 8
GRANULES = 2 * N_CHUNK
FIN_SLOTS = 8
TAKE = (
    (14, 15, 18, 20, 24, 26, 33, 38, 48, 50, 54, 59, 61, 64, 69, 71),
    (18, 20, 25, 26, 27, 28, 48, 50, 56, 59, 65, 68, 71, 72, 75, 76),
    (20, 23, 27, 32, 41, 43, 52, 57, 66, 70, 74, 75, 78, 80, 82, 85),
    (24, 29, 40, 52, 56, 67, 73, 74, 76, 77, 79, 81, 83, 84, 86, 87),
)
STEPS = TAKE + (tuple(TAKE[3][-1] + when for when in (-1, 0, 1, 2)),)
ROOT = 0.7978845608028654
CUBE = 0.044715


def gelu_hidden(pre):
    square = pre * pre
    bend = jnp.tanh(pre * (ROOT + (ROOT * CUBE) * square))
    half = 0.5 * pre
    return half + half * bend


def gelu_slope(pre):
    square = pre * pre
    bend = jnp.tanh(pre * (ROOT + (ROOT * CUBE) * square))
    tail = ((1.0 - bend * bend) * pre) * ((1.5 * ROOT * CUBE) * square + 0.5 * ROOT)
    return (0.5 + 0.5 * bend) + tail


def dot_nn(left, right):
    return lax.dot_general(left, right, (((1,), (0,)), ((), ())), preferred_element_type=F32)


def dot_nt(left, right):
    return lax.dot_general(left, right, (((1,), (1,)), ((), ())), preferred_element_type=F32)


class Dims:
    def __init__(self, tokens, width):
        self.tokens = tokens
        self.micro = tokens // 2
        self.width = width
        self.hidden = 4 * width
        self.rows = width // 8
        self.tile = 2 * self.rows
        self.half = width // 2
        self.quarter = width // 4
        unit = self.rows // 16
        self.row_a = max(8, (unit * 5) // 8 * 8)
        self.row_c = 4 * unit
        self.row_b = self.rows - self.row_a - self.row_c
        self.block = min(256, self.micro)
        self.span = min(512, width)


def kernel(dims, z2, z1, x2, x1, dy, win2, wo1, wo2, out,
           gin, xt, acc, dz, zbuf, wbuf, winbuf, ht, rcore,
           sums, r1a, r1b, r1c, s2a, s2b, s2c, r2a, r2b, r2c, s3ab, s3c, r3ab, r3c, s4ab, s4c, r4ab, r4c, fin, shard,
           zsem, wsem, winsem, xsem, gsem,
           core_send, core_recv, send1, recv1, send2, recv2, send3, recv3, send4, recv4,
           fin_send, fin_recv, fin_local, credit):
    rows, tile, width, half, quarter = dims.rows, dims.tile, dims.width, dims.half, dims.quarter
    micro, tokens, block, span = dims.micro, dims.tokens, dims.block, dims.span
    row_a, row_b, row_c = dims.row_a, dims.row_b, dims.row_c
    row_ab = row_a + row_b
    lanes = 128
    iz, iy, ix = lax.axis_index('dz'), lax.axis_index('dy'), lax.axis_index('dx')
    px, core = ix // 2, ix % 2
    zhi, zlo = iz // 2, iz % 2
    to_core = (iz, iy, px * 2 + (1 - core))
    to_x = (iz, iy, (1 - px) * 2 + core)
    to_xc = (iz, iy, (1 - px) * 2 + (1 - core))
    to_y = (iz, 1 - iy, ix)
    to_za = (zhi * 2 + (1 - zlo), iy, ix)
    to_zb = ((1 - zhi) * 2 + zlo, iy, ix)
    keep_x = pl.ds(pl.multiple_of(px * quarter, min(quarter, lanes)), quarter)
    send_x = pl.ds(pl.multiple_of((1 - px) * quarter, min(quarter, lanes)), quarter)
    CORE, A1, B1, C1, A2, B2, C2, AB3, C3, AB4, C4 = range(11)

    barrier = pltpu.get_barrier_semaphore()
    for peer in (to_core, to_x, to_xc, to_y, to_za, to_zb):
        pl.semaphore_signal(barrier, inc=1, device_id=peer, device_id_type=MESH)

    def order(num):
        k, t = num // 8, num % 8
        b, g, i = k // 4, (k // 2) % 2, k % 2
        plain_s, plain_p = t // 4, t % 4
        first = jnp.logical_or(t == 0, jnp.logical_and(t % 2 == 1, t < 7))
        mixed_s = jnp.where(first, 0, 1)
        mixed_p = jnp.where(first, (t + 1) // 2, jnp.where(t == 7, 3, t // 2 - 1))
        s = jnp.where(g == 0, mixed_s, plain_s)
        p = jnp.where(g == 0, mixed_p, plain_p)
        return k, b, i, g, s, p

    def piece_start(num):
        k, b, i, g, s, p = order(num)
        j = 2 * i + jnp.where(s == 0, 1 - core, core)
        slot = num % 3

        def from_block(zref, wref, with_win):
            @pl.when(g == 0)
            def _():
                for h in range(2):
                    col = pl.multiple_of((dims.hidden // 8) * (2 * p + h) + rows * j, rows)
                    pltpu.make_async_copy(zref.at[:, pl.ds(col, rows)], zbuf.at[slot, :, pl.ds(h * rows, rows)], zsem.at[slot]).start()

            @pl.when(g == 1)
            def _():
                col = pl.multiple_of(width * j + tile * p, tile)
                pltpu.make_async_copy(zref.at[:, pl.ds(col, tile)], zbuf.at[slot], zsem.at[slot]).start()
                pltpu.make_async_copy(wref.at[pl.ds(col, tile), :], wbuf.at[slot], wsem.at[slot]).start()
                if with_win:
                    pltpu.make_async_copy(win2.at[:, pl.ds(col, tile)], winbuf.at[slot], winsem.at[slot]).start()

        @pl.when(b == 0)
        def _():
            from_block(z2, wo2, True)

        @pl.when(b == 1)
        def _():
            from_block(z1, wo1, False)

    def piece_ahead(num):
        @pl.when(num + 2 < 8 * N_CHUNK)
        def _():
            piece_start(num + 2)

    def z_wait(num):
        pltpu.make_async_copy(z2.at[:, pl.ds(0, tile)], zbuf.at[num % 3], zsem.at[num % 3]).wait()

    def w_wait(num):
        pltpu.make_async_copy(wo2.at[pl.ds(0, tile), :], wbuf.at[num % 3], wsem.at[num % 3]).wait()

    def win_wait(num):
        pltpu.make_async_copy(win2.at[:, pl.ds(0, tile)], winbuf.at[num % 3], winsem.at[num % 3]).wait()

    def x_copy(xref, c):
        return pltpu.make_async_copy(xref.at[:, pl.ds(c * tile, tile)], dz.at[c % 2], xsem.at[c % 2])

    def core_copy(p):
        return pltpu.make_async_remote_copy(sums.at[8 + p % 2], rcore.at[p], core_send.at[p % 2], core_recv.at[p], device_id=to_core, device_id_type=MESH)

    def remote(src, dst, sends, recvs, peer):
        return pltpu.make_async_remote_copy(src, dst, sends, recvs, device_id=peer, device_id_type=MESH)

    def shift(q, part, size):
        return pl.ds(pl.multiple_of((q % 2) * half + part, min(quarter, lanes)), size)

    def phase1(q):
        base, r = (q // 2) % 2 * 4, q % 4
        return (
            remote(sums.at[pl.ds(base, 4), :, pl.ds(0, row_a), shift(q, (1 - px) * quarter, quarter)], r1a.at[r], send1.at[r, 0], recv1.at[r, 0], to_x),
            remote(sums.at[pl.ds(base + 2 * (1 - iy), 2), :, pl.ds(row_a, row_b), shift(q, 0, half)], r1b.at[r], send1.at[r, 1], recv1.at[r, 1], to_y),
            remote(sums.at[pl.ds(base, 4), 1 - zlo, pl.ds(row_ab, row_c), shift(q, 0, half)], r1c.at[r], send1.at[r, 2], recv1.at[r, 2], to_za),
        )

    def phase1_early(q, p):
        base, r = (q // 2) % 2 * 4, q % 4
        remote(sums.at[base + p, :, pl.ds(0, row_a), shift(q, (1 - px) * quarter, quarter)], r1a.at[r, p], send1.at[r, 0], recv1.at[r, 0], to_x).start()
        remote(sums.at[base + p, 1 - zlo, pl.ds(row_ab, row_c), shift(q, 0, half)], r1c.at[r, p], send1.at[r, 2], recv1.at[r, 2], to_za).start()

        @pl.when(p // 2 != iy)
        def _():
            remote(sums.at[base + p, :, pl.ds(row_a, row_b), shift(q, 0, half)], r1b.at[r, p % 2], send1.at[r, 1], recv1.at[r, 1], to_y).start()

    def phase1_claim(q, now):
        for kind in (A1, B1, C1):
            claim(kind, jnp.logical_and(q >= 4, now))

    def phase2(q):
        r = v = q % 4
        return (
            remote(s2a.at[v, pl.ds(2 * (1 - iy), 2)], r2a.at[r], send2.at[r, 0], recv2.at[r, 0], to_y),
            remote(s2b.at[v, :, :, :, send_x], r2b.at[r], send2.at[r, 1], recv2.at[r, 1], to_x),
            remote(s2c.at[v, :, 1 - zhi], r2c.at[r], send2.at[r, 2], recv2.at[r, 2], to_zb),
        )

    def phase3(q):
        r = v = q % 4
        return (
            remote(s3ab.at[v, :, 1 - zlo], r3ab.at[r], send3.at[r, 0], recv3.at[r, 0], to_za),
            remote(s3c.at[v, :, :, send_x], r3c.at[r], send3.at[r, 1], recv3.at[r, 1], to_x),
        )

    def phase4(q):
        r = v = q % 4
        return (
            remote(s4ab.at[v, 1 - zhi], r4ab.at[r], send4.at[r, 0], recv4.at[r, 0], to_zb),
            remote(s4c.at[v, 1 - iy], r4c.at[r], send4.at[r, 1], recv4.at[r, 1], to_y),
        )

    def grant(kind, peer, ok):
        @pl.when(ok)
        def _():
            pl.semaphore_signal(credit.at[kind], inc=1, device_id=peer, device_id_type=MESH)

    def claim(kind, ok):
        @pl.when(ok)
        def _():
            pl.semaphore_wait(credit.at[kind], 1)

    def shard_place(q):
        i, h = (q // 2) % 2, q % 2
        return 2 * i + core, pl.ds(pl.multiple_of(half * h + quarter * px, lanes), quarter)

    def owner_of(q):
        return q // 4

    def fin_start(q):
        f = q % FIN_SLOTS
        j, cols = shard_place(q)

        @pl.when(owner_of(q) == ix)
        def _():
            shard[j, :, cols] = fin[f]

        @pl.when(owner_of(q) != ix)
        def _():
            remote(fin.at[f], shard.at[j, :, cols], fin_send.at[f], fin_recv.at[(q // 2) % 2, q % 2, ix], (iz, iy, owner_of(q))).start()

    def fin_wait(q):
        f = q % FIN_SLOTS

        @pl.when(owner_of(q) != ix)
        def _():
            remote(fin.at[f], fin.at[f], fin_send.at[f], fin_recv.at[0, 0, ix], to_core).wait_send()

    def part_out(q):
        i, h = (q // 2) % 2, q % 2
        for d in range(4):
            @pl.when(ix != d)
            def _():
                remote(fin.at[0], fin.at[0], fin_send.at[0], fin_recv.at[i, h, d], to_core).wait_recv()
        for g in range(2):
            @pl.when(core == g)
            def _():
                for c in range(2):
                    j = 2 * i + c
                    for n in range(half // lanes):
                        strip = (half // lanes) * h + n
                        if g == 0:
                            place = out.at[pl.ds(pl.multiple_of(j * rows, rows), rows), strip, :]
                        else:
                            place = out.reshape(rows, 4, width // lanes, lanes).at[:, j, strip, :]
                        pltpu.make_async_copy(shard.at[j, :, pl.ds(pl.multiple_of(strip * lanes, lanes), lanes)], place, fin_local).start()

    def service(num):
        def stage_of(phase, act):
            due = num == STEPS[phase - 1][0]
            for when in STEPS[phase - 1][1:]:
                due = jnp.logical_or(due, num == when)

            @pl.when(due)
            def _():
                q = 0
                for when in STEPS[phase - 1]:
                    q = q + jnp.where(num > when, 1, 0)
                act(q, q % 4, q % 4, q < GRANULES - 4, q >= 4)

        def take4(q, r, v, more, later):
            ab, c = phase4(q)

            @pl.when(q >= FIN_SLOTS)
            def _():
                fin_wait(q - FIN_SLOTS)
            ab.wait()
            f = q % FIN_SLOTS
            fin[f, 0:row_ab, :] = s4ab[v, zhi] + r4ab[r]
            grant(AB4, to_zb, more)
            c.wait()
            fin[f, row_ab:rows, :] = s4c[v, iy] + r4c[r]
            grant(C4, to_y, more)
            fin_start(q)

        def take3(q, r, v, more, later):
            ab, c = phase3(q)
            ab4, c4 = phase4(q)
            ab.wait()
            s4ab[v] = s3ab[v, :, zlo] + r3ab[r]
            grant(AB3, to_za, more)
            claim(AB4, later)
            ab4.start()
            c.wait()
            s4c[v] = s3c[v, :, :, keep_x] + r3c[r]
            grant(C3, to_x, more)
            claim(C4, later)
            c4.start()

        def take2(q, r, v, more, later):
            a, b, c = phase2(q)
            ab3, c3 = phase3(q)
            a.wait()
            s3ab[v, :, :, 0:row_a, :] = s2a[v, pl.ds(2 * iy, 2)] + r2a[r]
            grant(A2, to_y, more)
            b.wait()
            s3ab[v, :, :, row_a:row_ab, :] = s2b[v, :, :, :, keep_x] + r2b[r]
            grant(B2, to_x, more)
            claim(AB3, later)
            ab3.start()
            c.wait()
            s3c[v] = s2c[v, :, zhi] + r2c[r]
            grant(C2, to_zb, more)
            claim(C3, later)
            c3.start()

        def take1(q, r, v, more, later):
            base = (q // 2) % 2 * 4
            a, b, c = phase1(q)
            a2, b2, c2 = phase2(q)
            a.wait()
            s2a[v] = sums[pl.ds(base, 4), :, 0:row_a, shift(q, px * quarter, quarter)] + r1a[r]
            grant(A1, to_x, more)
            claim(A2, later)
            a2.start()
            b.wait()
            s2b[v] = sums[pl.ds(base + 2 * iy, 2), :, row_a:row_ab, shift(q, 0, half)] + r1b[r]
            grant(B1, to_y, more)
            claim(B2, later)
            b2.start()
            c.wait()
            s2c[v] = (sums[pl.ds(base, 4), zlo, row_ab:rows, shift(q, 0, half)] + r1c[r]).reshape(2, 2, row_c, half)
            grant(C1, to_za, more)
            claim(C2, later)
            c2.start()

        stage_of(4, take4)
        stage_of(3, take3)
        stage_of(2, take2)
        stage_of(1, take1)

        def part(q, r, v, more, later):
            part_out(q)
        stage_of(5, part)

    def emit(to, into, source, cols, value):
        for h in range(2):
            sums[to, h, :, into] = value[h * rows:(h + 1) * rows] + rcore[source, h, :, cols]

    def tile_open(k, s, p):
        @pl.when(s == 0)
        def _():
            @pl.when(jnp.logical_or(k >= 1, p >= 2))
            def _():
                core_copy(p).wait_send()

        @pl.when(s == 1)
        def _():
            core_copy(p).wait_recv()

    def tile_close(k, s, p):
        @pl.when(s == 0)
        def _():
            claim(CORE, k >= 1)
            core_copy(p).start()

        @pl.when(s == 1)
        def _():
            grant(CORE, to_core, k < N_CHUNK - 1)

    def hidden_block(num, side, r):
        part = slice(r * block, (r + 1) * block)
        ht[side, :, part] = gelu_hidden(zbuf[num % 3, part, :].astype(F32)).astype(BF16).T

    def slope_block(num, side, r):
        part = slice(r * block, (r + 1) * block)
        back = dot_nt(gin[part, :], wbuf[num % 3])
        dz[side, part, :] = (back * gelu_slope(zbuf[num % 3, part, :].astype(F32))).astype(BF16)

    def rounded(value):
        return value.astype(BF16).astype(F32)

    n_block, n_span = tokens // block, width // span
    micros = [slice(m * micro, (m + 1) * micro) for m in range(2)]

    def tile_out(num):
        k, b, i, g, s, p = order(num)

        @pl.when(num % 32 == 0)
        def _():
            z_wait(num)
            for r in range(n_block):
                hidden_block(num, 0, r)

        @pl.when(num == 0)
        def _():
            first.wait()
            pl.semaphore_wait(barrier, 6)
        piece_ahead(num)
        more = num % 16 < 15

        @pl.when(more)
        def _():
            z_wait(num + 1)
        ahead = jnp.where(more, num + 1, num)
        side = num % 2
        tile_open(k, s, p)
        to = jnp.where(s == 0, 8 + p % 2, k % 2 * 4 + p)
        source = jnp.where(s == 0, 4, p)
        for n in range(n_span):
            cols = slice(n * span, (n + 1) * span)
            value = rounded(dot_nn(ht[side, :, micros[0]], gin[micros[0], cols])) + rounded(dot_nn(ht[side, :, micros[1]], gin[micros[1], cols]))
            for r in range(n * n_block // n_span, (n + 1) * n_block // n_span):
                hidden_block(ahead, 1 - side, r)
            emit(to, cols, source, cols, value)
        tile_close(k, s, p)

        @pl.when(s == 1)
        def _():
            for h in range(2):
                phase1_claim(2 * k + h, p == 0)
                phase1_early(2 * k + h, p)

    def tile_in(num):
        k, b, i, g, s, p = order(num)

        @pl.when(num % 32 == 16)
        def _():
            z_wait(num)
            w_wait(num)
            for r in range(n_block):
                slope_block(num, 0, r)
        piece_ahead(num)
        more = num % 16 < 15

        @pl.when(more)
        def _():
            z_wait(num + 1)
            w_wait(num + 1)
        ahead = jnp.where(more, num + 1, num)
        side = num % 2
        tile_open(k, s, p)
        source = jnp.where(s == 0, 4, p)
        for r in range(4):
            lines = slice(r * tile, (r + 1) * tile)
            to = jnp.where(s == 0, 8 + p % 2, k % 2 * 4 + r)
            into = pl.ds(pl.multiple_of(jnp.where(s == 0, r, p) * tile, tile), tile)
            spread = [range(r * n_block // 4 + m * n_block // 8, r * n_block // 4 + (m + 1) * n_block // 8) for m in range(2)]
            value = rounded(dot_nn(xt[lines, micros[0]], dz[side, micros[0], :]))
            for e in spread[0]:
                slope_block(ahead, 1 - side, e)
            value = value + rounded(dot_nn(xt[lines, micros[1]], dz[side, micros[1], :]))
            for e in spread[1]:
                slope_block(ahead, 1 - side, e)
            emit(to, into, source, lines, value)
        tile_close(k, s, p)

        @pl.when(jnp.logical_and(s == 1, p % 2 == 1))
        def _():
            q = 2 * k + p // 2
            phase1_claim(q, True)
            for copy in phase1(q):
                copy.start()

        @pl.when(b == 0)
        def _():
            win_wait(num)

            @pl.when(num == 16)
            def _():
                for r in range(n_block):
                    part = slice(r * block, (r + 1) * block)
                    acc[part, :] = gin[part, :].astype(F32) + dot_nt(dz[side, part, :], winbuf[num % 3])

            @pl.when(num != 16)
            def _():
                for r in range(n_block):
                    part = slice(r * block, (r + 1) * block)
                    acc[part, :] += dot_nt(dz[side, part, :], winbuf[num % 3])

    piece_start(0)
    first = pltpu.make_async_copy(dy, gin, gsem)
    first.start()
    piece_start(1)
    rcore[4] = jnp.zeros((2, rows, width), F32)

    def turn(xref):
        for c in range(4):
            x_copy(xref, c).wait()

            @pl.loop(0, n_block)
            def _(r):
                part = pl.ds(pl.multiple_of(r * block, block), block)
                xt[c * tile:(c + 1) * tile, part] = dz[c % 2, part, :].T
            if c < 2:
                x_copy(xref, c + 2).start()

    tiles = 8 * N_CHUNK

    @pl.loop(0, max(max(row) for row in STEPS) + 1)
    def _(num):
        @pl.when(num == N_CHUNK)
        def _():
            for c in range(2):
                x_copy(x2, c).start()

        @pl.when(num == tiles // 4)
        def _():
            turn(x2)

        @pl.when(num == tiles // 2)
        def _():
            for c in range(2):
                x_copy(x1, c).start()

            @pl.loop(0, n_block)
            def _(r):
                part = pl.ds(pl.multiple_of(r * block, block), block)
                gin[part, :] = acc[part, :].astype(BF16)

        @pl.when(num == 3 * tiles // 4)
        def _():
            turn(x1)

        @pl.when(jnp.logical_and(num < tiles, num % 32 < 16))
        def _():
            tile_out(num)

        @pl.when(jnp.logical_and(num < tiles, num % 32 >= 16))
        def _():
            tile_in(num)
        service(num)

    for p in range(2):
        core_copy(p).wait_send()
    pltpu.make_async_copy(out.at[pl.ds(0, 4 * rows)], out.at[pl.ds(0, 4 * rows)], fin_local).wait()
    for q in range(FIN_SLOTS):
        fin_wait(GRANULES - FIN_SLOTS + q)


def scratch(dims):
    t, w, r, h, q = dims.tokens, dims.width, dims.rows, dims.half, dims.quarter
    a, b, c = dims.row_a, dims.row_b, dims.row_c
    tile = dims.tile
    V, DMA = pltpu.VMEM, pltpu.SemaphoreType.DMA
    return [
        V((t, w), BF16), V((w, t), BF16), V((t, w), F32), V((2, t, tile), BF16), V((3, t, tile), BF16), V((3, tile, w), BF16), V((3, w, tile), BF16),
        V((2, tile, t), BF16), V((5, 2, r, w), F32),
        V((10, 2, r, w), F32), V((4, 4, 2, a, q), F32), V((4, 2, 2, b, h), F32), V((4, 4, c, h), F32),
        V((4, 4, 2, a, q), F32), V((4, 2, 2, b, h), F32), V((4, 2, 2, c, h), F32),
        V((4, 2, 2, a, q), F32), V((4, 2, 2, b, q), F32), V((4, 2, c, h), F32),
        V((4, 2, 2, a + b, q), F32), V((4, 2, c, h), F32), V((4, 2, a + b, q), F32), V((4, 2, c, q), F32),
        V((4, 2, a + b, q), F32), V((4, 2, c, q), F32), V((4, a + b, q), F32), V((4, c, q), F32), V((FIN_SLOTS, r, q), F32), V((4, r, w), F32),
        DMA((3,)), DMA((3,)), DMA((3,)), DMA((2,)), DMA,
        DMA((2,)), DMA((4,)), DMA((4, 3)), DMA((4, 3)), DMA((4, 3)), DMA((4, 3)), DMA((4, 2)), DMA((4, 2)), DMA((4, 2)), DMA((4, 2)),
        DMA((FIN_SLOTS,)), DMA((2, 2, 4)), DMA, pltpu.SemaphoreType.REGULAR((11,)),
    ]


def solution(mesh):
    row_spec = P(('dz', 'dy', 'dx'), None)
    full_spec = P(None, None)

    def per_device(act_one, pre_one, act_two, pre_two, grad_out, w_in_two, w_out_one, w_out_two):
        dims = Dims(*grad_out.shape)
        any_spec = pl.BlockSpec(memory_space=pl.ANY)
        shard = pl.pallas_call(
            functools.partial(kernel, dims),
            out_shape=jax.ShapeDtypeStruct((4 * dims.rows, dims.width // 128, 128), F32),
            in_specs=[any_spec] * 8,
            out_specs=any_spec,
            scratch_shapes=scratch(dims),
            compiler_params=pltpu.CompilerParams(collective_id=0, has_side_effects=True, vmem_limit_bytes=67043328),
        )(pre_two, pre_one, act_two, act_one, grad_out, w_in_two, w_out_one, w_out_two)
        return shard.reshape(-1)

    return jax.shard_map(per_device, mesh=mesh, in_specs=(row_spec,) * 5 + (full_spec,) * 3, out_specs=P(('dx', 'dy', 'dz')), check_vma=False)
```
